256 devices in a mesh: dom: 32 (over x, y, core), group: 8 (over z).
Axes of the slice: x: 4, y: 4, z: 8, core: 2. Of those that a mesh axis runs over, the one named last changes fastest.
Arguments:
- nodes: bfloat16 [256, 256, 128], P(('dom', 'group')), may hold values from -6 to 6
- edges: bfloat16 [256, 1536, 128], P(('dom', 'group')), may hold values from -6 to 6
- node_cot: bfloat16 [256, 256, 128], P(('dom', 'group')), may hold values from -6 to 6
- send_index: int32 [256, 4, 128], P(('dom', 'group')), may hold values from 0 to 255
- halo_count: int32 [256, 4], P(('dom', 'group')), may hold values from 0 to 128, as said below
- senders: int32 [256, 1536], P(('dom', 'group')), may hold values from 0 to 767, as said below
- receivers: int32 [256, 1536], P(('dom', 'group')), may hold values from 0 to 255, as said below
- edge_in_w: bfloat16 [2, 384, 128], replicated, may hold values from -0.3125 to 0.3125
- edge_out_w: bfloat16 [2, 128, 128], replicated, may hold values from -0.5 to 0.5
- node_in_w: bfloat16 [2, 256, 128], replicated, may hold values from -0.375 to 0.375
- node_out_w: bfloat16 [2, 128, 128], replicated, may hold values from -0.5 to 0.5
- biases: float32 [2, 4, 128], replicated, may hold values from -3 to 3
- gains: float32 [2, 2, 128], replicated, may hold values from 0.1 to 1.9
Outputs:
- nodes_out: bfloat16 [256, 256, 128], P(('dom', 'group'))
- node_grad: bfloat16 [256, 256, 128], P(('dom', 'group'))
- edge_grad: bfloat16 [256, 1536, 128], P(('dom', 'group'))
- edge_in_grad: float32 [2, 384, 128], replicated
- edge_out_grad: float32 [2, 128, 128], replicated
- node_in_grad: float32 [2, 256, 128], replicated
- node_out_grad: float32 [2, 128, 128], replicated
- bias_grad: float32 [2, 4, 128], replicated
- gain_grad: float32 [2, 2, 128], replicated
The draws below stay inside these ranges and needn't reach their ends.
Inputs may be any that keep to these rules, and one draw needn't show every extreme that they name: `halo_count`: slot order: from the lower then the upper partition along dom, then along group; 0 exactly where that neighbour does not exist; every slot reaches 128 on some partition. `senders`: below 256: a node of the partition; 256 + s: the s-th live halo row of the table, s below the partition's total halo_count. `receivers`: never fall along a partition's edges; within each aligned block of 512 edges they span fewer than 128 nodes.
All inputs are finite; a program needn't handle non-finite values.
Results may differ from the reference program's by a relative error of at most 0.02.
Values may be sent and summed in bfloat16 or wider, within the bound.
No kernel may reach another device: no remote copies, remote signals or barrier semaphores. Data moves between devices by JAX's collectives and lax.ppermute only.
A program may use at most 64 MiB of HBM per device.

```python
from functools import partial
import jax
import jax.numpy as jnp
from jax import lax

H = 128
L = 2
NODE_DEV = 256
HALO = 128
EDGE_DEV = 1536
PARTITIONS = 256
N_DOM = 32
N_GROUP = 8


def counts_table(key):
    base_key = jax.random.fold_in(key, 7)
    first_key, second_key = jax.random.split(base_key)
    partition = jnp.arange(PARTITIONS, dtype=jnp.int32)
    dom_place = partition // N_GROUP
    group_place = partition % N_GROUP
    present = jnp.stack([dom_place > 0, dom_place < N_DOM - 1, group_place > 0, group_place < N_GROUP - 1], axis=1)
    drawn = jax.random.randint(first_key, (PARTITIONS, 4), HALO // 4, HALO + 1)
    scores = jnp.where(present, jax.random.randint(second_key, (PARTITIONS, 4), 0, 1 << 30), -1)
    topmost = scores == jnp.max(scores, axis=0, keepdims=True)
    drawn = jnp.where(topmost, HALO, drawn)
    drawn = jnp.where((partition == N_GROUP + 1)[:, None], HALO, drawn)
    return jnp.where(present, drawn, 0).astype(jnp.int32)


def draw_halo_count(key, part):
    return counts_table(key)


def draw_senders(key, part):
    counts = counts_table(key)
    live_rows = jnp.sum(counts, axis=1).astype(jnp.int32)
    base_key = jax.random.fold_in(key, 11)
    local_key, pick_key, mode_key = jax.random.split(base_key, 3)
    local_ids = jax.random.randint(local_key, (PARTITIONS, EDGE_DEV), 0, NODE_DEV)
    picks = jax.random.randint(pick_key, (PARTITIONS, EDGE_DEV), 0, 1 << 30)
    remote_ids = NODE_DEV + picks % live_rows[:, None]
    choose_remote = jax.random.randint(mode_key, (PARTITIONS, EDGE_DEV), 0, 4) == 0
    chosen = jnp.where(choose_remote, remote_ids, local_ids).astype(jnp.int32)
    last_live = (NODE_DEV + live_rows - 1).astype(jnp.int32)
    first_edge = jnp.arange(EDGE_DEV, dtype=jnp.int32) == 0
    return jnp.where(first_edge[None, :], last_live[:, None], chosen).astype(jnp.int32)


def draw_receivers(key, part):
    base_key = jax.random.fold_in(key, 23)
    ramp_rows = jnp.arange(EDGE_DEV, dtype=jnp.int32) * NODE_DEV // EDGE_DEV
    jitter = jax.random.randint(base_key, (PARTITIONS, EDGE_DEV), 0, 32)
    return jnp.clip(jnp.sort(ramp_rows[None, :] + jitter, axis=1), 0, NODE_DEV - 1).astype(jnp.int32)


def touch_ends(array, key, least, top_value):
    index_at = [jax.random.randint(jax.random.fold_in(key, axis), (), 0, length) for axis, length in enumerate(array.shape)]
    main_axis = array.shape.index(max(array.shape))
    neighbour = index_at[:main_axis] + [(index_at[main_axis] + 1) % array.shape[main_axis]] + index_at[main_axis + 1:]
    return array.at[tuple(index_at)].set(least).at[tuple(neighbour)].set(top_value)


def levels(rng, dims, pieces, smallest, largest):
    gain, own = 1.0, jax.random.fold_in(rng, 6)
    for position, blocks in pieces:
        steps = jnp.exp(jax.random.uniform(jax.random.fold_in(own, position), (blocks,), jnp.float32, smallest / len(pieces), largest / len(pieces)))
        gain = gain * jnp.repeat(steps, dims[position] // blocks).reshape([-1 if axis == position else 1 for axis in range(len(dims))])
    return gain


def normal_values(rng, shape, width, most, shards=(), kind=jnp.bfloat16):
    gain = levels(rng, shape, shards, -0.22, 0.18) if shards else 1.0
    entries = jax.random.normal(rng, shape, jnp.float32) * width * gain
    return jnp.minimum(jnp.maximum(entries, -most), most).astype(kind)


def setup_inputs(seed: int = 0) -> dict:
    seeds = jax.random.split(jax.random.key(seed), 14)
    nodes = normal_values(seeds[0], (PARTITIONS, NODE_DEV, H), 1.0, 6.0, ((0, 256),))
    edges = normal_values(seeds[1], (PARTITIONS, EDGE_DEV, H), 1.0, 6.0, ((0, 256),))
    node_cot = normal_values(seeds[2], (PARTITIONS, NODE_DEV, H), 1.0, 6.0, ((0, 256),))
    send_index = touch_ends(jax.random.randint(seeds[3], (PARTITIONS, 4, HALO), 0, NODE_DEV), jax.random.fold_in(seeds[3], 1), 0, NODE_DEV - 1).astype(jnp.int32)
    halo_count = draw_halo_count(jax.random.fold_in(seeds[13], 71), 0)
    senders = draw_senders(jax.random.fold_in(seeds[13], 71), 0)
    receivers = draw_receivers(jax.random.fold_in(seeds[13], 71), 0)
    edge_in_w = normal_values(seeds[7], (L, 3 * H, H), (3 * H) ** -0.5, 0.3125)
    edge_out_w = normal_values(seeds[8], (L, H, H), H ** -0.5, 0.5)
    node_in_w = normal_values(seeds[9], (L, 2 * H, H), (2 * H) ** -0.5, 0.375)
    node_out_w = normal_values(seeds[10], (L, H, H), H ** -0.5, 0.5)
    biases = normal_values(seeds[11], (L, 4, H), 0.5, 3.0, (), jnp.float32)
    gains = jnp.clip(1.0 + 0.18 * jax.random.normal(seeds[12], (L, 2, H), jnp.float32), 0.1, 1.9)
    return dict(nodes=nodes, edges=edges, node_cot=node_cot, send_index=send_index, halo_count=halo_count, senders=senders, receivers=receivers, edge_in_w=edge_in_w, edge_out_w=edge_out_w, node_in_w=node_in_w, node_out_w=node_out_w, biases=biases, gains=gains)


def norm_rows(values, gain_row):
    centre = values - lax.optimization_barrier(jnp.mean(values, axis=-1, keepdims=True))
    spread = lax.optimization_barrier(jnp.mean(centre * centre, axis=-1, keepdims=True))
    return centre * lax.rsqrt(spread + 1e-05) * gain_row

def pack_halo(received, counts):
    halo_depth = received.shape[1]
    feat_width = received.shape[2]
    block_ends = jnp.cumsum(counts).astype(jnp.int32)
    block_starts = (block_ends - counts).astype(jnp.int32)
    positions = jnp.arange(4 * halo_depth, dtype=jnp.int32)
    block_of = lax.optimization_barrier(jnp.sum((positions[:, None] >= block_ends[None, :]).astype(jnp.int32), axis=1)).astype(jnp.int32)
    clamped = jnp.minimum(block_of, 3)
    selector = jnp.arange(4, dtype=jnp.int32)
    offsets = lax.optimization_barrier(jnp.sum(jnp.where(clamped[:, None] == selector[None, :], block_starts[None, :], 0), axis=1)).astype(jnp.int32)
    within_block = positions - offsets
    sources = clamped * halo_depth + jnp.clip(within_block, 0, halo_depth - 1)
    picked = received.reshape(4 * halo_depth, feat_width)[sources]
    return jnp.where((block_of < 4)[:, None], picked, jnp.zeros_like(picked))

def edge_update(weights, edge_rows, sent_feat, recv_feat):
    edge_in, edge_out, node_in, node_out, bias_rows, gain_rows = weights
    joined = jnp.concatenate([edge_rows, sent_feat, recv_feat], axis=1)
    hidden = jax.nn.silu(jnp.dot(joined, edge_in, preferred_element_type=jnp.float32) + bias_rows[0]).astype(jnp.bfloat16)
    mapped = jnp.dot(hidden, edge_out, preferred_element_type=jnp.float32) + bias_rows[1]
    return (edge_rows.astype(jnp.float32) + norm_rows(mapped, gain_rows[0])).astype(jnp.bfloat16)

def node_update(weights, node_vals, summed):
    edge_in, edge_out, node_in, node_out, bias_rows, gain_rows = weights
    joined = jnp.concatenate([node_vals.astype(jnp.bfloat16), summed.astype(jnp.bfloat16)], axis=1)
    hidden = jax.nn.silu(jnp.dot(joined, node_in, preferred_element_type=jnp.float32) + bias_rows[2]).astype(jnp.bfloat16)
    mapped = jnp.dot(hidden, node_out, preferred_element_type=jnp.float32) + bias_rows[3]
    return (node_vals + norm_rows(mapped, gain_rows[1])).astype(jnp.bfloat16)

def local_layer(weights, edge_rows, node_vals, received, counts, sender_ids, receiver_ids):
    table = jnp.concatenate([node_vals, pack_halo(received, counts)], axis=0)
    sent_feat = table[sender_ids].astype(jnp.bfloat16)
    recv_feat = table[receiver_ids].astype(jnp.bfloat16)
    edge_new = edge_update(weights, edge_rows, sent_feat, recv_feat)
    summed = jax.ops.segment_sum(edge_new.astype(jnp.float32), receiver_ids, num_segments=node_vals.shape[0])
    return (edge_new, node_update(weights, node_vals, summed))

def gather_rows(node_rows, send_rows):
    return node_rows.astype(jnp.float32)[send_rows]

def exchange_rows(node_all, send_index):
    sent_rows = jax.vmap(gather_rows)(node_all, send_index)
    grid_rows = sent_rows.reshape((N_DOM, N_GROUP) + sent_rows.shape[1:])
    zero_dom = jnp.zeros_like(grid_rows[:1, :, 0])
    zero_grp = jnp.zeros_like(grid_rows[:, :1, 0])
    slot_zero = jnp.concatenate([zero_dom, grid_rows[:-1, :, 0]], axis=0)
    slot_one = jnp.concatenate([grid_rows[1:, :, 1], zero_dom], axis=0)
    slot_two = jnp.concatenate([zero_grp, grid_rows[:, :-1, 2]], axis=1)
    slot_three = jnp.concatenate([grid_rows[:, 1:, 3], zero_grp], axis=1)
    return jnp.stack([slot_zero, slot_one, slot_two, slot_three], axis=2).reshape(sent_rows.shape)

def add_rows(returned, send_rows, node_count):
    return jax.ops.segment_sum(returned.reshape(-1, returned.shape[-1]), send_rows.reshape(-1), num_segments=node_count)

def scatter_back(cot_all, send_index, node_count):
    grid_rows = cot_all.reshape((N_DOM, N_GROUP) + cot_all.shape[1:])
    zero_dom = jnp.zeros_like(grid_rows[:1, :, 0])
    zero_grp = jnp.zeros_like(grid_rows[:, :1, 0])
    back_zero = jnp.concatenate([grid_rows[1:, :, 0], zero_dom], axis=0)
    back_one = jnp.concatenate([zero_dom, grid_rows[:-1, :, 1]], axis=0)
    back_two = jnp.concatenate([grid_rows[:, 1:, 2], zero_grp], axis=1)
    back_three = jnp.concatenate([zero_grp, grid_rows[:, :-1, 3]], axis=1)
    returned = jnp.stack([back_zero, back_one, back_two, back_three], axis=2).reshape(cot_all.shape)
    return jax.vmap(partial(add_rows, node_count=node_count))(returned, send_index)

def reference(nodes, edges, node_cot, send_index, halo_count, senders, receivers, edge_in_w, edge_out_w, node_in_w, node_out_w, biases, gains):
    layer_count = edge_in_w.shape[0]
    node_count = nodes.shape[1]
    node_all = nodes
    edge_all = edges
    saved_inputs = []
    for layer_index in range(layer_count):
        weights = (edge_in_w[layer_index], edge_out_w[layer_index], node_in_w[layer_index], node_out_w[layer_index], biases[layer_index], gains[layer_index])
        received = exchange_rows(node_all, send_index)
        saved_inputs.append((edge_all, node_all, received))

        def forward_one(carried, members, weights=weights):
            edge_vals, node_vals, halo_vals, counts, sender_ids, receiver_ids = members
            return (carried, local_layer(weights, edge_vals, node_vals.astype(jnp.float32), halo_vals, counts, sender_ids, receiver_ids))
        unused, (edge_all, node_all) = lax.scan(forward_one, jnp.zeros((), jnp.int32), (edge_all, node_all, received, halo_count, senders, receivers))
    node_cot_all = node_cot
    edge_cot_all = jnp.zeros_like(edges)
    layer_grads = [None] * layer_count
    for layer_index in reversed(range(layer_count)):
        weights = (edge_in_w[layer_index], edge_out_w[layer_index], node_in_w[layer_index], node_out_w[layer_index], biases[layer_index], gains[layer_index])
        edge_in_all, node_in_all, received = saved_inputs[layer_index]

        def backward_one(totals, members, weights=weights):
            edge_vals, node_vals, halo_vals, counts, sender_ids, receiver_ids, edge_cot, node_cot_rows = members

            def layer_call(params, edge_arg, node_arg, halo_arg):
                return local_layer(params, edge_arg, node_arg, halo_arg, counts, sender_ids, receiver_ids)
            outputs, pullback = jax.vjp(layer_call, weights, edge_vals, node_vals.astype(jnp.float32), halo_vals)
            weight_cot, edge_back, node_back, halo_back = pullback((edge_cot, node_cot_rows))
            totals = tuple((running + leaf_val.astype(jnp.float32) for running, leaf_val in zip(totals, weight_cot)))
            return (totals, (edge_back, node_back, halo_back))
        initial = tuple((jnp.zeros(leaf_val.shape, jnp.float32) for leaf_val in weights))
        totals, (edge_cot_all, node_back_all, halo_back_all) = lax.scan(backward_one, initial, (edge_in_all, node_in_all, received, halo_count, senders, receivers, edge_cot_all, node_cot_all))
        node_back_all = node_back_all + scatter_back(halo_back_all, send_index, node_count)
        node_cot_all = node_back_all.astype(jnp.bfloat16)
        layer_grads[layer_index] = totals
    grad_scale = (N_DOM * N_GROUP * node_count) ** (-0.5)
    stacked = tuple((jnp.stack([layer_grads[layer_index][member] for layer_index in range(layer_count)]) * grad_scale for member in range(6)))
    return (node_all, node_cot_all, edge_cot_all, stacked[0], stacked[1], stacked[2], stacked[3], stacked[4], stacked[5])
```

```python
import jax
import jax.numpy as jnp
from jax import lax
from jax.experimental import pallas as pl
from jax.experimental.pallas import tpu as pltpu
from jax.sharding import PartitionSpec as P

H = 128
BLOCK = 512
GRAD_ROWS = 1024
VMEM_LIMIT = 28 << 20
F32 = jnp.float32
BF16 = jnp.bfloat16


def mm(a, b):
    return lax.dot_general(a, b, (((1,), (0,)), ((), ())), preferred_element_type=F32)


def mm_nt(a, b):
    return lax.dot_general(a, b, (((1,), (1,)), ((), ())), preferred_element_type=F32)


def mm_tn(a, b):
    return lax.dot_general(a, b, (((0,), (0,)), ((), ())), preferred_element_type=F32)


def column(row):
    return jnp.transpose(jnp.broadcast_to(row, (8, row.shape[1])))[:, :1]


def hot(mask):
    return jnp.where(mask, 1.0, 0.0).astype(BF16)


def pick_rows(row, width):
    col = column(row)
    return hot(lax.broadcasted_iota(jnp.int32, (row.shape[1], width), 1) == col)


def spread_rows(row, width):
    return hot(lax.broadcasted_iota(jnp.int32, (width, row.shape[1]), 0) == row)


def slot_ids(ids, counts):
    out = ids
    end = 256
    for k in range(3):
        end = end + counts[k]
        out = out + jnp.where(ids >= end, 128 - counts[k], 0)
    return out


def silu_parts(pre):
    sig = 0.5 * jnp.tanh(0.5 * pre) + 0.5
    return pre * sig, sig * (1.0 + pre * (1.0 - sig))


def norm_parts(mapped):
    centre = mapped - jnp.mean(mapped, axis=-1, keepdims=True)
    spread = jnp.mean(centre * centre, axis=-1, keepdims=True)
    scale = lax.rsqrt(spread + 1e-05)
    return centre * scale, scale


def norm_back(cot, xhat, scale, gain):
    grad = cot * gain
    first = jnp.mean(grad, axis=-1, keepdims=True)
    second = jnp.mean(grad * xhat, axis=-1, keepdims=True)
    return scale * (grad - first - xhat * second)


def total(x):
    return jnp.sum(x, axis=0, keepdims=True)


def write_sends(send_ref, rows, outs):
    for k in range(4):
        picked = mm(pick_rows(send_ref[k : k + 1, :], 256), rows)
        outs[k][...] = picked.astype(BF16)


def add_returns(send_ref, rets):
    out = jnp.zeros((256, H), F32)
    for k in range(4):
        out = out + mm(spread_rows(send_ref[k : k + 1, :], 256), rets[k][...])
    return out


def sends_kernel(send_ref, x_ref, o0, o1, o2, o3):
    write_sends(send_ref, x_ref[...], (o0, o1, o2, o3))


def edge_forward(counts, snd_ref, rcv_ref, table, e_ref, w1, w2, b_ref, g_ref, joined, hidden, slope, xhat, scale, e_new, agg):
    agg[...] = jnp.zeros((256, H), F32)

    def step(i, carry):
        rows = pl.ds(pl.multiple_of(i * BLOCK, BLOCK), BLOCK)
        ids = slot_ids(snd_ref[i], counts)
        sent = mm(pick_rows(ids, 768), table[...]).astype(BF16)
        recv = mm(pick_rows(rcv_ref[i], 256), table[0:256, :]).astype(BF16)
        joined[rows, 0:128] = e_ref[rows, :]
        joined[rows, 128:256] = sent
        joined[rows, 256:384] = recv
        pre = mm(joined[rows, :], w1[...]) + b_ref[0:1, :]
        act, slo = silu_parts(pre)
        act = act.astype(BF16)
        hidden[rows, :] = act
        slope[rows, :] = slo
        xh, sc = norm_parts(mm(act, w2[...]) + b_ref[1:2, :])
        xhat[rows, :] = xh
        scale[rows, :] = sc
        new = (e_ref[rows, :].astype(F32) + xh * g_ref[0:1, :]).astype(BF16)
        if e_new is not None:
            e_new[rows, :] = new
        agg[...] += mm(spread_rows(rcv_ref[i], 256), new)
        return carry

    lax.fori_loop(0, e_ref.shape[0] // BLOCK, step, 0)


def node_forward(x, agg, wn1, wn2, b_ref, g_ref):
    joined = jnp.concatenate([x, agg.astype(BF16)], axis=1)
    act, slo = silu_parts(mm(joined, wn1[...]) + b_ref[2:3, :])
    act = act.astype(BF16)
    xh, sc = norm_parts(mm(act, wn2[...]) + b_ref[3:4, :])
    new = (x.astype(F32) + xh * g_ref[1:2, :]).astype(BF16)
    return new, (joined, act, slo, xh, sc)


def node_backward(cot, saved, wn1, wn2, g_ref, grads):
    joined, act, slo, xh, sc = saved
    cot = cot.astype(F32)
    back = norm_back(cot, xh, sc, g_ref[1:2, :])
    back_b = back.astype(BF16)
    dpre = mm_nt(back_b, wn2[...]).astype(BF16).astype(F32) * slo
    dpre_b = dpre.astype(BF16)
    djoined = mm_nt(dpre_b, wn1[...]).astype(BF16)
    grads[512:768, :] = mm_tn(joined, dpre_b).astype(BF16)
    grads[768:896, :] = mm_tn(act, back_b).astype(BF16)
    small = (total(dpre), total(back), total(cot * xh))
    return cot + djoined[:, 0:128].astype(F32), djoined[:, 128:256], small


def edge_backward(counts, snd_ref, rcv_ref, w1, w2, g_ref, joined, hidden, slope, xhat, scale, dagg, e_cot, e_grad, acc, acc1, acc2, sums, grads):
    acc[...] = jnp.zeros(acc.shape, F32)
    acc1[...] = jnp.zeros(acc1.shape, F32)
    acc2[...] = jnp.zeros(acc2.shape, F32)
    sums[...] = jnp.zeros(sums.shape, F32)

    def step(i, carry):
        rows = pl.ds(pl.multiple_of(i * BLOCK, BLOCK), BLOCK)
        cot = mm(pick_rows(rcv_ref[i], 256), dagg)
        if e_cot is not None:
            cot = (cot + e_cot[rows, :].astype(F32)).astype(BF16).astype(F32)
        xh = xhat[rows, :]
        back = norm_back(cot, xh, scale[rows, :], g_ref[0:1, :])
        back_b = back.astype(BF16)
        dpre = mm_nt(back_b, w2[...]).astype(BF16).astype(F32) * slope[rows, :]
        dpre_b = dpre.astype(BF16)
        djoined = mm_nt(dpre_b, w1[...]).astype(BF16)
        e_grad[rows, :] = (cot + djoined[:, 0:128].astype(F32)).astype(BF16)
        ids = slot_ids(snd_ref[i], counts)
        acc[...] += mm(spread_rows(ids, 768), djoined[:, 128:256])
        acc[0:256, :] += mm(spread_rows(rcv_ref[i], 256), djoined[:, 256:384])
        acc1[...] += mm_tn(dpre_b, joined[rows, :])
        acc2[...] += mm_tn(back_b, hidden[rows, :])
        sums[0:1, :] += total(dpre)
        sums[1:2, :] += total(back)
        sums[2:3, :] += total(cot * xh)
        return carry

    lax.fori_loop(0, joined.shape[0] // BLOCK, step, 0)
    for k in range(3):
        grads[128 * k : 128 * k + 128, :] = jnp.transpose(acc1[:, 128 * k : 128 * k + 128]).astype(BF16)
    grads[384:512, :] = jnp.transpose(acc2[...]).astype(BF16)


def write_small(grads, sums, small):
    tail = jnp.concatenate(
        [sums[0:2, :], small[0], small[1], sums[2:3, :], small[2], jnp.zeros((122, H), F32)], axis=0
    )
    grads[896:1024, :] = tail.astype(BF16)


def first_kernel(
    cnt, snd_ref, rcv_ref, send_ref, x_ref, r0, r1, r2, r3, e_ref, w1, w2, wn1, wn2, b_ref, g_ref,
    joined, hidden, slope, xhat, scale, e_new, agg_b, x_new, o0, o1, o2, o3, table, agg,
):
    counts = (cnt[0], cnt[1], cnt[2])
    table[0:256, :] = x_ref[...]
    for k, r in enumerate((r0, r1, r2, r3)):
        table[256 + 128 * k : 384 + 128 * k, :] = r[...]
    edge_forward(counts, snd_ref, rcv_ref, table, e_ref, w1, w2, b_ref, g_ref, joined, hidden, slope, xhat, scale, e_new, agg)
    new, saved = node_forward(x_ref[...], agg[...], wn1, wn2, b_ref, g_ref)
    agg_b[...] = agg[...].astype(BF16)
    x_new[...] = new
    write_sends(send_ref, new, (o0, o1, o2, o3))


def last_kernel(
    cnt, snd_ref, rcv_ref, x_ref, r0, r1, r2, r3, e_ref, w1, w2, wn1, wn2, b_ref, g_ref, cot_ref,
    x_new, e_grad, x_grad, c0, c1, c2, c3, grads,
    table, agg, joined, hidden, slope, xhat, scale, acc, acc1, acc2, sums,
):
    counts = (cnt[0], cnt[1], cnt[2])
    table[0:256, :] = x_ref[...]
    for k, r in enumerate((r0, r1, r2, r3)):
        table[256 + 128 * k : 384 + 128 * k, :] = r[...]
    edge_forward(counts, snd_ref, rcv_ref, table, e_ref, w1, w2, b_ref, g_ref, joined, hidden, slope, xhat, scale, None, agg)
    new, saved = node_forward(x_ref[...], agg[...], wn1, wn2, b_ref, g_ref)
    x_new[...] = new
    dx, dagg, small = node_backward(cot_ref[...], saved, wn1, wn2, g_ref, grads)
    edge_backward(counts, snd_ref, rcv_ref, w1, w2, g_ref, joined, hidden, slope, xhat, scale, dagg, None, e_grad, acc, acc1, acc2, sums, grads)
    write_small(grads, sums, small)
    x_grad[...] = dx + acc[0:256, :]
    for k, c in enumerate((c0, c1, c2, c3)):
        c[...] = acc[256 + 128 * k : 384 + 128 * k, :].astype(BF16)


def back_kernel(
    cnt, snd_ref, rcv_ref, send_ref, x_ref, agg_b, own_ref, t0, t1, t2, t3, joined, hidden, slope, xhat, scale, e_cot,
    w1, w2, wn1, wn2, b_ref, g_ref,
    e_grad, x_grad, c0, c1, c2, c3, grads, acc, acc1, acc2, sums,
):
    counts = (cnt[0], cnt[1], cnt[2])
    cot = (own_ref[...] + add_returns(send_ref, (t0, t1, t2, t3))).astype(BF16)
    new, saved = node_forward(x_ref[...], agg_b[...], wn1, wn2, b_ref, g_ref)
    dx, dagg, small = node_backward(cot, saved, wn1, wn2, g_ref, grads)
    edge_backward(counts, snd_ref, rcv_ref, w1, w2, g_ref, joined, hidden, slope, xhat, scale, dagg, e_cot, e_grad, acc, acc1, acc2, sums, grads)
    write_small(grads, sums, small)
    x_grad[...] = dx + acc[0:256, :]
    for k, c in enumerate((c0, c1, c2, c3)):
        c[...] = acc[256 + 128 * k : 384 + 128 * k, :].astype(BF16)


def finish_kernel(send_ref, own_ref, t0, t1, t2, t3, o_ref):
    o_ref[...] = (own_ref[...] + add_returns(send_ref, (t0, t1, t2, t3))).astype(BF16)


def shape(*dims, dtype=F32):
    return jax.ShapeDtypeStruct(dims, dtype)


def call(kernel, outs, scratch, args, name):
    smem = pl.BlockSpec(memory_space=pltpu.SMEM)
    vmem = pl.BlockSpec(memory_space=pltpu.VMEM)
    specs = [smem if a.ndim == 1 else vmem for a in args]
    return pl.pallas_call(
        kernel,
        out_shape=outs,
        in_specs=specs,
        out_specs=[vmem] * len(outs),
        scratch_shapes=[pltpu.VMEM(s.shape, s.dtype) for s in scratch],
        compiler_params=pltpu.CompilerParams(vmem_limit_bytes=VMEM_LIMIT),
        name=name,
    )(*args)


def steps_of(axis):
    size = lax.axis_size(axis)
    up = [(i, i + 1) for i in range(size - 1)]
    down = [(i + 1, i) for i in range(size - 1)]
    return up, down


def exchange(blocks, back):
    up_d, down_d = steps_of("dom")
    up_g, down_g = steps_of("group")
    plan = (("dom", up_d), ("dom", down_d), ("group", up_g), ("group", down_g))
    if back:
        plan = (plan[1], plan[0], plan[3], plan[2])
    return [lax.ppermute(b, axis, pairs) for b, (axis, pairs) in zip(blocks, plan)]


def copies(x, axis):
    many = jnp.broadcast_to(x[None], (lax.axis_size(axis), *x.shape))
    return lax.all_to_all(many, axis, split_axis=0, concat_axis=0, tiled=True)


def reduce_grads(packed):
    tiles = packed.reshape(lax.axis_size("dom"), -1, H)
    tiles = lax.all_to_all(tiles, "dom", split_axis=0, concat_axis=0, tiled=True)
    share = jnp.sum(tiles.astype(F32), axis=0).astype(BF16)
    share = jnp.sum(copies(share, "group").astype(F32), axis=0).astype(BF16)
    return copies(share, "dom").reshape(-1, H)


def shards(nodes, edges, node_cot, send_index, halo_count, senders, receivers, edge_in_w, edge_out_w, node_in_w, node_out_w, biases, gains):
    x0 = nodes[0]
    e0 = edges[0]
    send = send_index[0]
    counts = halo_count[0]
    n_edge = e0.shape[0]
    snd = senders[0].reshape(n_edge // BLOCK, 1, BLOCK)
    rcv = receivers[0].reshape(n_edge // BLOCK, 1, BLOCK)
    weights = [(edge_in_w[l], edge_out_w[l], node_in_w[l], node_out_w[l], biases[l], gains[l]) for l in range(2)]
    rows4 = [shape(H, H, dtype=BF16)] * 4
    residuals = [
        shape(n_edge, 3 * H, dtype=BF16),
        shape(n_edge, H, dtype=BF16),
        shape(n_edge, H),
        shape(n_edge, H),
        shape(n_edge, 1),
    ]
    accs = [shape(768, H), shape(H, 3 * H), shape(H, H), shape(8, H)]
    table = shape(768, H, dtype=BF16)

    sent = call(sends_kernel, rows4, [], (send, x0), "sends")
    got = exchange(sent, False)
    out = call(
        first_kernel,
        residuals + [shape(n_edge, H, dtype=BF16), shape(256, H, dtype=BF16), shape(256, H, dtype=BF16)] + rows4,
        [table, shape(256, H)],
        (counts, snd, rcv, send, x0, *got, e0, *weights[0]),
        "layer0",
    )
    saved, (e1, agg0, x1), sent = out[:5], out[5:8], out[8:]
    got = exchange(sent, False)
    out = call(
        last_kernel,
        [shape(256, H, dtype=BF16), shape(n_edge, H, dtype=BF16), shape(256, H)] + rows4 + [shape(GRAD_ROWS, H, dtype=BF16)],
        [table, shape(256, H)] + residuals + accs,
        (counts, snd, rcv, x1, *got, e1, *weights[1], node_cot[0]),
        "layer1",
    )
    nodes_out, e_cot, own = out[:3]
    grads1 = out[7]
    back = exchange(out[3:7], True)
    out = call(
        back_kernel,
        [shape(n_edge, H, dtype=BF16), shape(256, H)] + rows4 + [shape(GRAD_ROWS, H, dtype=BF16)],
        accs,
        (counts, snd, rcv, send, x0, agg0, own, *back, *saved, e_cot, *weights[0]),
        "back0",
    )
    edge_grad, own = out[:2]
    grads0 = out[6]
    back = exchange(out[2:6], True)
    (node_grad,) = call(finish_kernel, [shape(256, H, dtype=BF16)], [], (send, own, *back), "finish")

    scale = (lax.axis_size("dom") * lax.axis_size("group") * x0.shape[0]) ** (-0.5)
    whole = [reduce_grads(g).astype(F32) * scale for g in (grads0, grads1)]
    cuts = ((0, 384), (384, 512), (512, 768), (768, 896), (896, 900), (900, 902))
    grads = [jnp.stack([w[a:b] for w in whole]) for a, b in cuts]
    return (nodes_out[None], node_grad[None], edge_grad[None], *grads)


def solution(mesh):
    part = ("dom", "group")
    in_specs = (P(part),) * 7 + (P(),) * 6
    out_specs = (P(part),) * 3 + (P(),) * 6
    return jax.shard_map(shards, mesh=mesh, in_specs=in_specs, out_specs=out_specs, check_vma=False)
```

```python
from functools import partial

import jax
import jax.numpy as jnp
from jax import lax
from jax.experimental import pallas as pl
from jax.experimental.pallas import tpu as pltpu
from jax.sharding import PartitionSpec as P

H = 128
BLOCK = 512
GRAD_ROWS = 1024
VMEM_LIMIT = 28 << 20
CUTS = ((0, 384), (384, 512), (512, 768), (768, 896), (896, 900), (900, 902))
F32 = jnp.float32
BF16 = jnp.bfloat16


def mm(a, b):
    return lax.dot_general(a, b, (((1,), (0,)), ((), ())), preferred_element_type=F32)


def mm_nt(a, b):
    return lax.dot_general(a, b, (((1,), (1,)), ((), ())), preferred_element_type=F32)


def mm_tn(a, b):
    return lax.dot_general(a, b, (((0,), (0,)), ((), ())), preferred_element_type=F32)


def column(row):
    return jnp.transpose(jnp.broadcast_to(row, (8, row.shape[1])))[:, :1]


def hot(mask):
    return jnp.where(mask, 1.0, 0.0).astype(BF16)


def pick_rows(row, width):
    col = column(row)
    return hot(lax.broadcasted_iota(jnp.int32, (row.shape[1], width), 1) == col)


def spread_rows(row, width):
    return hot(lax.broadcasted_iota(jnp.int32, (width, row.shape[1]), 0) == row)


def slot_ids(ids, counts):
    out = ids
    end = 256
    for k in range(3):
        end = end + counts[k]
        out = out + jnp.where(ids >= end, 128 - counts[k], 0)
    return out


def silu_parts(pre):
    sig = 0.5 * jnp.tanh(0.5 * pre) + 0.5
    return pre * sig, sig * (1.0 + pre * (1.0 - sig))


def norm_parts(mapped):
    centre = mapped - jnp.mean(mapped, axis=-1, keepdims=True)
    spread = jnp.mean(centre * centre, axis=-1, keepdims=True)
    scale = lax.rsqrt(spread + 1e-05)
    return centre * scale, scale


def norm_back(cot, xhat, scale, gain):
    grad = cot * gain
    first = jnp.mean(grad, axis=-1, keepdims=True)
    second = jnp.mean(grad * xhat, axis=-1, keepdims=True)
    return scale * (grad - first - xhat * second)


def total(x):
    return jnp.sum(x, axis=0, keepdims=True)


def sides():
    p = lax.axis_index("dom") % 2
    g = lax.axis_index("group") % 2
    return (p, 1 - p), (1 - p, p), (2 + g, 3 - g), (3 - g, 2 + g)


def write_sends(send_ref, rows, outs):
    for (src, _), out in zip(sides(), outs):
        picked = mm(pick_rows(send_ref[pl.ds(src, 1), :], 256), rows)
        out[...] = picked.astype(BF16)


def add_returns(send_ref, rets):
    out = jnp.zeros((256, H), F32)
    for (src, _), ret in zip(sides(), rets):
        out = out + mm(spread_rows(send_ref[pl.ds(src, 1), :], 256), ret[...])
    return out


def slot_rows(slot):
    return pl.ds(pl.multiple_of(256 + 128 * slot, 128), 128)


def fill_table(table, x_ref, got):
    table[0:256, :] = x_ref[...]
    for (_, dst), r in zip(sides(), got):
        table[slot_rows(dst), :] = r[...]


def write_backs(acc, outs):
    for (_, dst), out in zip(sides(), outs):
        out[...] = acc[slot_rows(dst), :].astype(BF16)


def fetch(pairs, sems):
    copies = [pltpu.make_async_copy(src, dst, sems.at[i]) for i, (src, dst) in enumerate(pairs)]
    for c in copies:
        c.start()
    return copies


def sends_kernel(send_hbm, x_hbm, o0, o1, o2, o3, send_ref, x_ref, sems):
    for c in fetch(((send_hbm, send_ref), (x_hbm, x_ref)), sems):
        c.wait()
    write_sends(send_ref, x_ref[...], (o0, o1, o2, o3))


def load_kernel(cnt, token, *refs):
    sems = refs[-1]
    n = (len(refs) - 1) // 2
    copies = fetch(tuple(zip(refs[:n], refs[n:-1])), sems)
    for c in copies:
        c.wait()
    snd_ref = refs[n]
    snd_ref[...] = slot_ids(snd_ref[...], (cnt[0], cnt[1], cnt[2]))


def edge_forward(snd_ref, rcv_ref, table, e_ref, w1, w2, b_ref, g_ref, joined, hidden, slope, xhat, scale, e_new, agg):
    agg[...] = jnp.zeros((256, H), F32)

    def step(i, carry):
        rows = pl.ds(pl.multiple_of(i * BLOCK, BLOCK), BLOCK)
        ids = snd_ref[i]
        sent = mm(pick_rows(ids, 768), table[...]).astype(BF16)
        recv = mm(pick_rows(rcv_ref[i], 256), table[0:256, :]).astype(BF16)
        joined[rows, 0:128] = e_ref[rows, :]
        joined[rows, 128:256] = sent
        joined[rows, 256:384] = recv
        pre = mm(joined[rows, :], w1[...]) + b_ref[0:1, :]
        act, slo = silu_parts(pre)
        act = act.astype(BF16)
        hidden[rows, :] = act
        slope[rows, :] = slo
        xh, sc = norm_parts(mm(act, w2[...]) + b_ref[1:2, :])
        xhat[rows, :] = xh
        scale[rows, :] = sc
        new = (e_ref[rows, :].astype(F32) + xh * g_ref[0:1, :]).astype(BF16)
        if e_new is not None:
            e_new[rows, :] = new
        agg[...] += mm(spread_rows(rcv_ref[i], 256), new)
        return carry

    lax.fori_loop(0, e_ref.shape[0] // BLOCK, step, 0)


def node_forward(x, agg, wn1, wn2, b_ref, g_ref):
    joined = jnp.concatenate([x, agg.astype(BF16)], axis=1)
    act, slo = silu_parts(mm(joined, wn1[...]) + b_ref[2:3, :])
    act = act.astype(BF16)
    xh, sc = norm_parts(mm(act, wn2[...]) + b_ref[3:4, :])
    new = (x.astype(F32) + xh * g_ref[1:2, :]).astype(BF16)
    return new, (joined, act, slo, xh, sc)


def node_backward(cot, saved, wn1, wn2, g_ref, grads):
    joined, act, slo, xh, sc = saved
    cot = cot.astype(F32)
    back = norm_back(cot, xh, sc, g_ref[1:2, :])
    back_b = back.astype(BF16)
    dpre = mm_nt(back_b, wn2[...]).astype(BF16).astype(F32) * slo
    dpre_b = dpre.astype(BF16)
    djoined = mm_nt(dpre_b, wn1[...]).astype(BF16)
    grads[512:768, :] = mm_tn(joined, dpre_b).astype(BF16)
    grads[768:896, :] = mm_tn(act, back_b).astype(BF16)
    small = (total(dpre), total(back), total(cot * xh))
    return cot + djoined[:, 0:128].astype(F32), djoined[:, 128:256], small


def edge_backward(snd_ref, rcv_ref, w1, w2, g_ref, joined, hidden, slope, xhat, scale, dagg, e_cot, e_grad, acc, acc1, acc2, sums, grads):
    acc[...] = jnp.zeros(acc.shape, F32)
    acc1[...] = jnp.zeros(acc1.shape, F32)
    acc2[...] = jnp.zeros(acc2.shape, F32)
    sums[...] = jnp.zeros(sums.shape, F32)

    def step(i, carry):
        rows = pl.ds(pl.multiple_of(i * BLOCK, BLOCK), BLOCK)
        cot = mm(pick_rows(rcv_ref[i], 256), dagg)
        if e_cot is not None:
            cot = (cot + e_cot[rows, :].astype(F32)).astype(BF16).astype(F32)
        xh = xhat[rows, :]
        back = norm_back(cot, xh, scale[rows, :], g_ref[0:1, :])
        back_b = back.astype(BF16)
        dpre = mm_nt(back_b, w2[...]).astype(BF16).astype(F32) * slope[rows, :]
        dpre_b = dpre.astype(BF16)
        djoined = mm_nt(dpre_b, w1[...]).astype(BF16)
        e_grad[rows, :] = (cot + djoined[:, 0:128].astype(F32)).astype(BF16)
        ids = snd_ref[i]
        acc[...] += mm(spread_rows(ids, 768), djoined[:, 128:256])
        acc[0:256, :] += mm(spread_rows(rcv_ref[i], 256), djoined[:, 256:384])
        acc1[...] += mm_tn(dpre_b, joined[rows, :])
        acc2[...] += mm_tn(back_b, hidden[rows, :])
        sums[0:1, :] += total(dpre)
        sums[1:2, :] += total(back)
        sums[2:3, :] += total(cot * xh)
        return carry

    lax.fori_loop(0, joined.shape[0] // BLOCK, step, 0)
    for k in range(3):
        grads[128 * k : 128 * k + 128, :] = jnp.transpose(acc1[:, 128 * k : 128 * k + 128]).astype(BF16)
    grads[384:512, :] = jnp.transpose(acc2[...]).astype(BF16)


def write_small(grads, sums, small):
    tail = jnp.concatenate(
        [sums[0:2, :], small[0], small[1], sums[2:3, :], small[2], jnp.zeros((GRAD_ROWS - 902, H), F32)], axis=0
    )
    grads[896:GRAD_ROWS, :] = tail.astype(BF16)


def first_kernel(
    snd_ref, rcv_ref, send_ref, x_ref, r0, r1, r2, r3, e_ref, w1, w2, wn1, wn2, b_ref, g_ref,
    joined, hidden, slope, xhat, scale, e_new, agg_b, x_new, o0, o1, o2, o3, table, agg,
):
    w1, w2, wn1, wn2, b_ref, g_ref = (r.at[0] for r in (w1, w2, wn1, wn2, b_ref, g_ref))
    fill_table(table, x_ref, (r0, r1, r2, r3))
    edge_forward(snd_ref, rcv_ref, table, e_ref, w1, w2, b_ref, g_ref, joined, hidden, slope, xhat, scale, e_new, agg)
    new, saved = node_forward(x_ref[...], agg[...], wn1, wn2, b_ref, g_ref)
    agg_b[...] = agg[...].astype(BF16)
    x_new[...] = new
    write_sends(send_ref, new, (o0, o1, o2, o3))


def last_kernel(
    snd_ref, rcv_ref, x_ref, r0, r1, r2, r3, e_ref, w1, w2, wn1, wn2, b_ref, g_ref, cot_ref,
    x_new, e_grad, x_grad, c0, c1, c2, c3, grads,
    table, agg, joined, hidden, slope, xhat, scale, acc, acc1, acc2, sums,
):
    w1, w2, wn1, wn2, b_ref, g_ref = (r.at[1] for r in (w1, w2, wn1, wn2, b_ref, g_ref))
    fill_table(table, x_ref, (r0, r1, r2, r3))
    edge_forward(snd_ref, rcv_ref, table, e_ref, w1, w2, b_ref, g_ref, joined, hidden, slope, xhat, scale, None, agg)
    new, saved = node_forward(x_ref[...], agg[...], wn1, wn2, b_ref, g_ref)
    x_new[...] = new
    dx, dagg, small = node_backward(cot_ref[...], saved, wn1, wn2, g_ref, grads)
    edge_backward(snd_ref, rcv_ref, w1, w2, g_ref, joined, hidden, slope, xhat, scale, dagg, None, e_grad, acc, acc1, acc2, sums, grads)
    write_small(grads, sums, small)
    x_grad[...] = dx + acc[0:256, :]
    write_backs(acc, (c0, c1, c2, c3))


def back_kernel(
    snd_ref, rcv_ref, send_ref, x_ref, agg_b, own_ref, t0, t1, t2, t3, joined, hidden, slope, xhat, scale, e_cot, late,
    w1, w2, wn1, wn2, b_ref, g_ref,
    e_grad, x_grad, c0, c1, c2, c3, grads, acc, acc1, acc2, sums,
):
    w1, w2, wn1, wn2, b_ref, g_ref = (r.at[0] for r in (w1, w2, wn1, wn2, b_ref, g_ref))
    grads[GRAD_ROWS:, :] = late[...]
    cot = (own_ref[...] + add_returns(send_ref, (t0, t1, t2, t3))).astype(BF16)
    new, saved = node_forward(x_ref[...], agg_b[...], wn1, wn2, b_ref, g_ref)
    dx, dagg, small = node_backward(cot, saved, wn1, wn2, g_ref, grads)
    edge_backward(snd_ref, rcv_ref, w1, w2, g_ref, joined, hidden, slope, xhat, scale, dagg, e_cot, e_grad, acc, acc1, acc2, sums, grads)
    write_small(grads, sums, small)
    x_grad[...] = dx + acc[0:256, :]
    write_backs(acc, (c0, c1, c2, c3))


def finish_kernel(send_ref, own_ref, t0, t1, t2, t3, o_ref):
    o_ref[...] = (own_ref[...] + add_returns(send_ref, (t0, t1, t2, t3))).astype(BF16)


def shape(*dims, dtype=F32):
    return jax.ShapeDtypeStruct(dims, dtype)


SMEM = pltpu.SMEM
VMEM = pltpu.VMEM
HBM = pltpu.HBM


def call(kernel, outs, scratch, args, name, spaces=None, sems=0):
    spaces = spaces or [VMEM] * len(args)
    args = [pltpu.with_memory_space_constraint(a, m) if m is HBM else a for a, m in zip(args, spaces)]
    extra = [pltpu.SemaphoreType.DMA((sems,))] if sems else []
    return pl.pallas_call(
        kernel,
        out_shape=outs,
        in_specs=[pl.BlockSpec(memory_space=m) for m in spaces],
        out_specs=[pl.BlockSpec(memory_space=VMEM)] * len(outs),
        scratch_shapes=[VMEM(s.shape, s.dtype) for s in scratch] + extra,
        compiler_params=pltpu.CompilerParams(vmem_limit_bytes=VMEM_LIMIT),
        name=name,
    )(*args)


def swaps(axis, first):
    size = lax.axis_size(axis)
    return [p for i in range(first, size - 1, 2) for p in ((i, i + 1), (i + 1, i))]


def exchange(blocks):
    plan = (("dom", 0), ("dom", 1), ("group", 0), ("group", 1))
    return [lax.ppermute(b, axis, swaps(axis, first)) for b, (axis, first) in zip(blocks, plan)]


def fold_kernel(x_ref, o_ref):
    out = jnp.sum(x_ref[...].astype(F32), axis=0).astype(BF16)
    for k in range(o_ref.shape[0]):
        o_ref[k] = out


def unpack_kernel(scale, x_ref, *outs):
    for out, (a, b) in zip(outs, CUTS):
        for l in range(2):
            out[l] = x_ref[GRAD_ROWS * l + a : GRAD_ROWS * l + b, :].astype(F32) * scale


def swap_tiles(x, axis):
    return lax.all_to_all(x, axis, split_axis=0, concat_axis=0, tiled=True)


def reduce_grads(packed, scale):
    dom, group = lax.axis_size("dom"), lax.axis_size("group")
    rows = packed.shape[0] // dom
    tiles = swap_tiles(packed.reshape(dom, rows, H), "dom")
    (tiles,) = call(fold_kernel, [shape(group, rows, H, dtype=BF16)], [], (tiles,), "fold_dom")
    tiles = swap_tiles(tiles, "group")
    (tiles,) = call(fold_kernel, [shape(dom, rows, H, dtype=BF16)], [], (tiles,), "fold_group")
    whole = swap_tiles(tiles, "dom").reshape(dom * rows, H)
    return call(partial(unpack_kernel, scale), [shape(2, b - a, H) for a, b in CUTS], [], (whole,), "unpack")


def shards(nodes, edges, node_cot, send_index, halo_count, senders, receivers, edge_in_w, edge_out_w, node_in_w, node_out_w, biases, gains):
    x0 = nodes[0]
    e0 = edges[0]
    send = send_index[0]
    counts = halo_count[0]
    n_edge = e0.shape[0]
    snd = senders[0].reshape(n_edge // BLOCK, 1, BLOCK)
    rcv = receivers[0].reshape(n_edge // BLOCK, 1, BLOCK)
    weights = (edge_in_w, edge_out_w, node_in_w, node_out_w, biases, gains)
    rows4 = [shape(H, H, dtype=BF16)] * 4
    residuals = [
        shape(n_edge, 3 * H, dtype=BF16),
        shape(n_edge, H, dtype=BF16),
        shape(n_edge, H),
        shape(n_edge, H),
        shape(n_edge, 1),
    ]
    accs = [shape(768, H), shape(H, 3 * H), shape(H, H), shape(8, H)]
    table = shape(768, H, dtype=BF16)

    *sent, send, x0 = call(
        sends_kernel,
        rows4 + [shape(4, H, dtype=jnp.int32), shape(256, H, dtype=BF16)],
        [],
        (send, x0),
        "sends",
        [HBM, HBM],
        2,
    )
    raw = (snd, rcv, e0, node_cot[0], *weights)
    loaded = call(
        load_kernel,
        [shape(*a.shape, dtype=a.dtype) for a in raw],
        [],
        (counts, sent[0], *raw),
        "load",
        [SMEM, VMEM] + [HBM] * len(raw),
        len(raw),
    )
    snd, rcv, e0, cot, *weights = loaded
    got = exchange(sent)
    out = call(
        first_kernel,
        residuals + [shape(n_edge, H, dtype=BF16), shape(256, H, dtype=BF16), shape(256, H, dtype=BF16)] + rows4,
        [table, shape(256, H)],
        (snd, rcv, send, x0, *got, e0, *weights),
        "layer0",
    )
    saved, (e1, agg0, x1), sent = out[:5], out[5:8], out[8:]
    got = exchange(sent)
    out = call(
        last_kernel,
        [shape(256, H, dtype=BF16), shape(n_edge, H, dtype=BF16), shape(256, H)] + rows4 + [shape(GRAD_ROWS, H, dtype=BF16)],
        [table, shape(256, H)] + residuals + accs,
        (snd, rcv, x1, *got, e1, *weights, cot),
        "layer1",
    )
    nodes_out, e_cot, own = out[:3]
    grads1 = out[7]
    back = exchange(out[3:7])
    out = call(
        back_kernel,
        [shape(n_edge, H, dtype=BF16), shape(256, H)] + rows4 + [shape(2 * GRAD_ROWS, H, dtype=BF16)],
        accs,
        (snd, rcv, send, x0, agg0, own, *back, *saved, e_cot, grads1, *weights),
        "back0",
    )
    edge_grad, own = out[:2]
    packed = out[6]
    back = exchange(out[2:6])
    (node_grad,) = call(finish_kernel, [shape(256, H, dtype=BF16)], [], (send, own, *back), "finish")

    scale = (lax.axis_size("dom") * lax.axis_size("group") * x0.shape[0]) ** (-0.5)
    grads = reduce_grads(packed, scale)
    return (nodes_out[None], node_grad[None], edge_grad[None], *grads)


def solution(mesh):
    part = ("dom", "group")
    in_specs = (P(part),) * 7 + (P(),) * 6
    out_specs = (P(part),) * 3 + (P(),) * 6
    return jax.shard_map(shards, mesh=mesh, in_specs=in_specs, out_specs=out_specs, check_vma=False)
```

```python
from functools import partial

import jax
import jax.numpy as jnp
from jax import lax
from jax.experimental import pallas as pl
from jax.experimental.pallas import tpu as pltpu
from jax.sharding import PartitionSpec as P

H = 128
BLOCK = 512
GRAD_ROWS = 1024
VMEM_LIMIT = 28 << 20
CUTS = ((0, 384), (384, 512), (512, 768), (768, 896), (896, 900), (900, 902))
F32 = jnp.float32
BF16 = jnp.bfloat16


def mm(a, b):
    return lax.dot_general(a, b, (((1,), (0,)), ((), ())), preferred_element_type=F32)


def mm_nt(a, b):
    return lax.dot_general(a, b, (((1,), (1,)), ((), ())), preferred_element_type=F32)


def mm_tn(a, b):
    return lax.dot_general(a, b, (((0,), (0,)), ((), ())), preferred_element_type=F32)


def column(row):
    return jnp.transpose(jnp.broadcast_to(row, (8, row.shape[1])))[:, :1]


def hot(mask):
    return jnp.where(mask, 1.0, 0.0).astype(BF16)


def pick_rows(row, width):
    col = column(row)
    return hot(lax.broadcasted_iota(jnp.int32, (row.shape[1], width), 1) == col)


def spread_rows(row, width):
    return hot(lax.broadcasted_iota(jnp.int32, (width, row.shape[1]), 0) == row)


def slot_ids(ids, counts):
    out = ids
    end = 256
    for k in range(3):
        end = end + counts[k]
        out = out + jnp.where(ids >= end, 128 - counts[k], 0)
    return out


def silu_parts(pre):
    sig = 0.5 * jnp.tanh(0.5 * pre) + 0.5
    return pre * sig, sig * (1.0 + pre * (1.0 - sig))


def norm_parts(mapped):
    centre = mapped - jnp.mean(mapped, axis=-1, keepdims=True)
    spread = jnp.mean(centre * centre, axis=-1, keepdims=True)
    scale = lax.rsqrt(spread + 1e-05)
    return centre * scale, scale


def norm_back(cot, xhat, scale, gain):
    grad = cot * gain
    first = jnp.mean(grad, axis=-1, keepdims=True)
    second = jnp.mean(grad * xhat, axis=-1, keepdims=True)
    return scale * (grad - first - xhat * second)


def total(x):
    return jnp.sum(x, axis=0, keepdims=True)


def sides():
    p = lax.axis_index("dom") % 2
    g = lax.axis_index("group") % 2
    return (p, 1 - p), (1 - p, p), (2 + g, 3 - g), (3 - g, 2 + g)


def write_sends(send_ref, rows, outs):
    for (src, _), out in zip(sides(), outs):
        picked = mm(pick_rows(send_ref[pl.ds(src, 1), :], 256), rows)
        out[...] = picked.astype(BF16)


def add_returns(send_ref, rets):
    out = jnp.zeros((256, H), F32)
    for (src, _), ret in zip(sides(), rets):
        out = out + mm(spread_rows(send_ref[pl.ds(src, 1), :], 256), ret[...])
    return out


def slot_rows(slot):
    return pl.ds(pl.multiple_of(256 + 128 * slot, 128), 128)


def fill_table(table, x_ref, got):
    table[0:256, :] = x_ref[...]
    for (_, dst), r in zip(sides(), got):
        table[slot_rows(dst), :] = r[...]


def write_backs(acc, outs):
    for (_, dst), out in zip(sides(), outs):
        out[...] = acc[slot_rows(dst), :].astype(BF16)


def fetch(pairs, sems):
    copies = [pltpu.make_async_copy(src, dst, sems.at[i]) for i, (src, dst) in enumerate(pairs)]
    for c in copies:
        c.start()
    return copies


def sends_kernel(send_hbm, x_hbm, o0, o1, o2, o3, send_ref, x_ref, sems):
    for c in fetch(((send_hbm, send_ref), (x_hbm, x_ref)), sems):
        c.wait()
    write_sends(send_ref, x_ref[...], (o0, o1, o2, o3))


def load_kernel(cnt, token, *refs):
    sems = refs[-1]
    n = (len(refs) - 1) // 2
    copies = fetch(tuple(zip(refs[:n], refs[n:-1])), sems)
    for c in copies:
        c.wait()
    snd_ref = refs[n]
    snd_ref[...] = slot_ids(snd_ref[...], (cnt[0], cnt[1], cnt[2]))


def edge_forward(snd_ref, rcv_ref, table, e_ref, w1, w2, b_ref, g_ref, joined, hidden, slope, xhat, scale, e_new, agg):
    agg[...] = jnp.zeros((256, H), F32)

    def step(i, carry):
        rows = pl.ds(pl.multiple_of(i * BLOCK, BLOCK), BLOCK)
        ids = snd_ref[i]
        sent = mm(pick_rows(ids, 768), table[...]).astype(BF16)
        recv = mm(pick_rows(rcv_ref[i], 256), table[0:256, :]).astype(BF16)
        joined[rows, 0:128] = e_ref[rows, :]
        joined[rows, 128:256] = sent
        joined[rows, 256:384] = recv
        pre = mm(joined[rows, :], w1[...]) + b_ref[0:1, :]
        act, slo = silu_parts(pre)
        act = act.astype(BF16)
        hidden[rows, :] = act
        slope[rows, :] = slo
        xh, sc = norm_parts(mm(act, w2[...]) + b_ref[1:2, :])
        xhat[rows, :] = xh
        scale[rows, :] = sc
        new = (e_ref[rows, :].astype(F32) + xh * g_ref[0:1, :]).astype(BF16)
        if e_new is not None:
            e_new[rows, :] = new
        agg[...] += mm(spread_rows(rcv_ref[i], 256), new)
        return carry

    lax.fori_loop(0, e_ref.shape[0] // BLOCK, step, 0, unroll=True)


def node_forward(x, agg, wn1, wn2, b_ref, g_ref):
    joined = jnp.concatenate([x, agg.astype(BF16)], axis=1)
    act, slo = silu_parts(mm(joined, wn1[...]) + b_ref[2:3, :])
    act = act.astype(BF16)
    xh, sc = norm_parts(mm(act, wn2[...]) + b_ref[3:4, :])
    new = (x.astype(F32) + xh * g_ref[1:2, :]).astype(BF16)
    return new, (joined, act, slo, xh, sc)


def node_backward(cot, saved, wn1, wn2, g_ref, grads):
    joined, act, slo, xh, sc = saved
    cot = cot.astype(F32)
    back = norm_back(cot, xh, sc, g_ref[1:2, :])
    back_b = back.astype(BF16)
    dpre = mm_nt(back_b, wn2[...]).astype(BF16).astype(F32) * slo
    dpre_b = dpre.astype(BF16)
    djoined = mm_nt(dpre_b, wn1[...]).astype(BF16)
    grads[512:768, :] = mm_tn(joined, dpre_b).astype(BF16)
    grads[768:896, :] = mm_tn(act, back_b).astype(BF16)
    small = (total(dpre), total(back), total(cot * xh))
    return cot + djoined[:, 0:128].astype(F32), djoined[:, 128:256], small


def edge_backward(snd_ref, rcv_ref, w1, w2, g_ref, joined, hidden, slope, xhat, scale, dagg, e_cot, e_grad, acc, acc1, acc2, sums, grads):
    acc[...] = jnp.zeros(acc.shape, F32)
    acc1[...] = jnp.zeros(acc1.shape, F32)
    acc2[...] = jnp.zeros(acc2.shape, F32)
    sums[...] = jnp.zeros(sums.shape, F32)

    def step(i, carry):
        rows = pl.ds(pl.multiple_of(i * BLOCK, BLOCK), BLOCK)
        cot = mm(pick_rows(rcv_ref[i], 256), dagg)
        if e_cot is not None:
            cot = (cot + e_cot[rows, :].astype(F32)).astype(BF16).astype(F32)
        xh = xhat[rows, :]
        back = norm_back(cot, xh, scale[rows, :], g_ref[0:1, :])
        back_b = back.astype(BF16)
        dpre = mm_nt(back_b, w2[...]).astype(BF16).astype(F32) * slope[rows, :]
        dpre_b = dpre.astype(BF16)
        djoined = mm_nt(dpre_b, w1[...]).astype(BF16)
        e_grad[rows, :] = (cot + djoined[:, 0:128].astype(F32)).astype(BF16)
        ids = snd_ref[i]
        acc[...] += mm(spread_rows(ids, 768), djoined[:, 128:256])
        acc[0:256, :] += mm(spread_rows(rcv_ref[i], 256), djoined[:, 256:384])
        acc1[...] += mm_tn(dpre_b, joined[rows, :])
        acc2[...] += mm_tn(back_b, hidden[rows, :])
        sums[0:1, :] += total(dpre)
        sums[1:2, :] += total(back)
        sums[2:3, :] += total(cot * xh)
        return carry

    lax.fori_loop(0, joined.shape[0] // BLOCK, step, 0, unroll=True)
    for k in range(3):
        grads[128 * k : 128 * k + 128, :] = jnp.transpose(acc1[:, 128 * k : 128 * k + 128]).astype(BF16)
    grads[384:512, :] = jnp.transpose(acc2[...]).astype(BF16)


def write_small(grads, sums, small):
    tail = jnp.concatenate(
        [sums[0:2, :], small[0], small[1], sums[2:3, :], small[2], jnp.zeros((GRAD_ROWS - 902, H), F32)], axis=0
    )
    grads[896:GRAD_ROWS, :] = tail.astype(BF16)


def first_kernel(
    snd_ref, rcv_ref, send_ref, x_ref, r0, r1, r2, r3, e_ref, w1, w2, wn1, wn2, b_ref, g_ref,
    joined, hidden, slope, xhat, scale, e_new, agg_b, x_new, o0, o1, o2, o3, table, agg,
):
    w1, w2, wn1, wn2, b_ref, g_ref = (r.at[0] for r in (w1, w2, wn1, wn2, b_ref, g_ref))
    fill_table(table, x_ref, (r0, r1, r2, r3))
    edge_forward(snd_ref, rcv_ref, table, e_ref, w1, w2, b_ref, g_ref, joined, hidden, slope, xhat, scale, e_new, agg)
    new, saved = node_forward(x_ref[...], agg[...], wn1, wn2, b_ref, g_ref)
    agg_b[...] = agg[...].astype(BF16)
    x_new[...] = new
    write_sends(send_ref, new, (o0, o1, o2, o3))


def last_kernel(
    snd_ref, rcv_ref, x_ref, r0, r1, r2, r3, e_ref, w1, w2, wn1, wn2, b_ref, g_ref, cot_ref,
    x_new, e_grad, x_grad, c0, c1, c2, c3, grads,
    table, agg, joined, hidden, slope, xhat, scale, acc, acc1, acc2, sums,
):
    w1, w2, wn1, wn2, b_ref, g_ref = (r.at[1] for r in (w1, w2, wn1, wn2, b_ref, g_ref))
    fill_table(table, x_ref, (r0, r1, r2, r3))
    edge_forward(snd_ref, rcv_ref, table, e_ref, w1, w2, b_ref, g_ref, joined, hidden, slope, xhat, scale, None, agg)
    new, saved = node_forward(x_ref[...], agg[...], wn1, wn2, b_ref, g_ref)
    x_new[...] = new
    dx, dagg, small = node_backward(cot_ref[...], saved, wn1, wn2, g_ref, grads)
    edge_backward(snd_ref, rcv_ref, w1, w2, g_ref, joined, hidden, slope, xhat, scale, dagg, None, e_grad, acc, acc1, acc2, sums, grads)
    write_small(grads, sums, small)
    x_grad[...] = dx + acc[0:256, :]
    write_backs(acc, (c0, c1, c2, c3))


def back_kernel(
    snd_ref, rcv_ref, send_ref, x_ref, agg_b, own_ref, t0, t1, t2, t3, joined, hidden, slope, xhat, scale, e_cot, late,
    w1, w2, wn1, wn2, b_ref, g_ref,
    e_grad, x_grad, c0, c1, c2, c3, grads, acc, acc1, acc2, sums,
):
    w1, w2, wn1, wn2, b_ref, g_ref = (r.at[0] for r in (w1, w2, wn1, wn2, b_ref, g_ref))
    grads[GRAD_ROWS:, :] = late[...]
    cot = (own_ref[...] + add_returns(send_ref, (t0, t1, t2, t3))).astype(BF16)
    new, saved = node_forward(x_ref[...], agg_b[...], wn1, wn2, b_ref, g_ref)
    dx, dagg, small = node_backward(cot, saved, wn1, wn2, g_ref, grads)
    edge_backward(snd_ref, rcv_ref, w1, w2, g_ref, joined, hidden, slope, xhat, scale, dagg, e_cot, e_grad, acc, acc1, acc2, sums, grads)
    write_small(grads, sums, small)
    x_grad[...] = dx + acc[0:256, :]
    write_backs(acc, (c0, c1, c2, c3))


def finish_kernel(send_ref, own_ref, t0, t1, t2, t3, o_ref):
    o_ref[...] = (own_ref[...] + add_returns(send_ref, (t0, t1, t2, t3))).astype(BF16)


def shape(*dims, dtype=F32):
    return jax.ShapeDtypeStruct(dims, dtype)


SMEM = pltpu.SMEM
VMEM = pltpu.VMEM
HBM = pltpu.HBM


def call(kernel, outs, scratch, args, name, spaces=None, sems=0):
    spaces = spaces or [VMEM] * len(args)
    args = [pltpu.with_memory_space_constraint(a, m) if m is HBM else a for a, m in zip(args, spaces)]
    extra = [pltpu.SemaphoreType.DMA((sems,))] if sems else []
    return pl.pallas_call(
        kernel,
        out_shape=outs,
        in_specs=[pl.BlockSpec(memory_space=m) for m in spaces],
        out_specs=[pl.BlockSpec(memory_space=VMEM)] * len(outs),
        scratch_shapes=[VMEM(s.shape, s.dtype) for s in scratch] + extra,
        compiler_params=pltpu.CompilerParams(vmem_limit_bytes=VMEM_LIMIT),
        name=name,
    )(*args)


def swaps(axis, first):
    size = lax.axis_size(axis)
    return [p for i in range(first, size - 1, 2) for p in ((i, i + 1), (i + 1, i))]


def exchange(blocks):
    plan = (("dom", 0), ("dom", 1), ("group", 0), ("group", 1))
    return [lax.ppermute(b, axis, swaps(axis, first)) for b, (axis, first) in zip(blocks, plan)]


def fold_kernel(x_ref, *refs):
    o_ref = refs[-1]
    out = jnp.sum(x_ref[...].astype(F32), axis=0).astype(BF16)
    for k in range(o_ref.shape[0]):
        o_ref[k] = out


def unpack_kernel(scale, x_ref, *outs):
    for out, (a, b) in zip(outs, CUTS):
        for l in range(2):
            out[l] = x_ref[GRAD_ROWS * l + a : GRAD_ROWS * l + b, :].astype(F32) * scale


def swap_tiles(x, axis):
    return lax.all_to_all(x, axis, split_axis=0, concat_axis=0, tiled=True)


def reduce_grads(packed, scale, first, second):
    dom, group = lax.axis_size("dom"), lax.axis_size("group")
    rows = packed.shape[0] // dom
    tiles = swap_tiles(packed.reshape(dom, rows, H), "dom")
    (tiles,) = call(fold_kernel, [shape(group, rows, H, dtype=BF16)], [], (tiles, *first), "fold_dom")
    tiles = swap_tiles(tiles, "group")
    (tiles,) = call(fold_kernel, [shape(dom, rows, H, dtype=BF16)], [], (tiles, *second), "fold_group")
    whole = swap_tiles(tiles, "dom").reshape(dom * rows, H)
    return call(partial(unpack_kernel, scale), [shape(2, b - a, H) for a, b in CUTS], [], (whole,), "unpack")


def shards(nodes, edges, node_cot, send_index, halo_count, senders, receivers, edge_in_w, edge_out_w, node_in_w, node_out_w, biases, gains):
    x0 = nodes[0]
    e0 = edges[0]
    send = send_index[0]
    counts = halo_count[0]
    n_edge = e0.shape[0]
    snd = senders[0].reshape(n_edge // BLOCK, 1, BLOCK)
    rcv = receivers[0].reshape(n_edge // BLOCK, 1, BLOCK)
    weights = (edge_in_w, edge_out_w, node_in_w, node_out_w, biases, gains)
    rows4 = [shape(H, H, dtype=BF16)] * 4
    residuals = [
        shape(n_edge, 3 * H, dtype=BF16),
        shape(n_edge, H, dtype=BF16),
        shape(n_edge, H),
        shape(n_edge, H),
        shape(n_edge, 1),
    ]
    accs = [shape(768, H), shape(H, 3 * H), shape(H, H), shape(8, H)]
    table = shape(768, H, dtype=BF16)

    *sent, send, x0 = call(
        sends_kernel,
        rows4 + [shape(4, H, dtype=jnp.int32), shape(256, H, dtype=BF16)],
        [],
        (send, x0),
        "sends",
        [HBM, HBM],
        2,
    )
    raw = (snd, rcv, e0, node_cot[0], *weights)
    loaded = call(
        load_kernel,
        [shape(*a.shape, dtype=a.dtype) for a in raw],
        [],
        (counts, sent[0], *raw),
        "load",
        [SMEM, VMEM] + [HBM] * len(raw),
        len(raw),
    )
    snd, rcv, e0, cot, *weights = loaded
    got = exchange(sent)
    out = call(
        first_kernel,
        residuals + [shape(n_edge, H, dtype=BF16), shape(256, H, dtype=BF16), shape(256, H, dtype=BF16)] + rows4,
        [table, shape(256, H)],
        (snd, rcv, send, x0, *got, e0, *weights),
        "layer0",
    )
    saved, (e1, agg0, x1), sent = out[:5], out[5:8], out[8:]
    got = exchange(sent)
    out = call(
        last_kernel,
        [shape(256, H, dtype=BF16), shape(n_edge, H, dtype=BF16), shape(256, H)] + rows4 + [shape(GRAD_ROWS, H, dtype=BF16)],
        [table, shape(256, H)] + residuals + accs,
        (snd, rcv, x1, *got, e1, *weights, cot),
        "layer1",
    )
    nodes_out, e_cot, own = out[:3]
    grads1 = out[7]
    back = exchange(out[3:7])
    out = call(
        back_kernel,
        [shape(n_edge, H, dtype=BF16), shape(256, H)] + rows4 + [shape(2 * GRAD_ROWS, H, dtype=BF16)],
        accs,
        (snd, rcv, send, x0, agg0, own, *back, *saved, e_cot, grads1, *weights),
        "back0",
    )
    edge_grad, own = out[:2]
    packed = out[6]
    back = exchange(out[2:6])
    (node_grad,) = call(finish_kernel, [shape(256, H, dtype=BF16)], [], (send, own, *back), "finish")

    scale = (lax.axis_size("dom") * lax.axis_size("group") * x0.shape[0]) ** (-0.5)
    grads = reduce_grads(packed, scale, back[:2], back[2:])
    return (nodes_out[None], node_grad[None], edge_grad[None], *grads)


def solution(mesh):
    part = ("dom", "group")
    in_specs = (P(part),) * 7 + (P(),) * 6
    out_specs = (P(part),) * 3 + (P(),) * 6
    return jax.shard_map(shards, mesh=mesh, in_specs=in_specs, out_specs=out_specs, check_vma=False)
```

```python
from functools import partial

import jax
import jax.numpy as jnp
from jax import lax
from jax.experimental import pallas as pl
from jax.experimental.pallas import tpu as pltpu
from jax.sharding import PartitionSpec as P

H = 128
BLOCK = 512
GRAD_ROWS = 1024
VMEM_LIMIT = 28 << 20
CUTS = ((0, 384), (384, 512), (512, 768), (768, 896), (896, 900), (900, 902))
F32 = jnp.float32
BF16 = jnp.bfloat16


def mm(a, b):
    return lax.dot_general(a, b, (((1,), (0,)), ((), ())), preferred_element_type=F32)


def mm_nt(a, b):
    return lax.dot_general(a, b, (((1,), (1,)), ((), ())), preferred_element_type=F32)


def mm_tn(a, b):
    return lax.dot_general(a, b, (((0,), (0,)), ((), ())), preferred_element_type=F32)


def column(row):
    return jnp.transpose(jnp.broadcast_to(row, (8, row.shape[1])))[:, :1]


def hot(mask):
    return jnp.where(mask, 1.0, 0.0).astype(BF16)


def pick_rows(row, width):
    col = column(row)
    return hot(lax.broadcasted_iota(jnp.int32, (row.shape[1], width), 1) == col)


def spread_rows(row, width):
    return hot(lax.broadcasted_iota(jnp.int32, (width, row.shape[1]), 0) == row)


def slot_ids(ids, counts):
    out = ids
    end = 256
    for k in range(3):
        end = end + counts[k]
        out = out + jnp.where(ids >= end, 128 - counts[k], 0)
    return out


def silu_parts(pre):
    sig = 0.5 * jnp.tanh(0.5 * pre) + 0.5
    return pre * sig, sig * (1.0 + pre * (1.0 - sig))


def norm_parts(mapped):
    centre = mapped - jnp.mean(mapped, axis=-1, keepdims=True)
    spread = jnp.mean(centre * centre, axis=-1, keepdims=True)
    scale = lax.rsqrt(spread + 1e-05)
    return centre * scale, scale


def norm_back(cot, xhat, scale, gain):
    grad = cot * gain
    first = jnp.mean(grad, axis=-1, keepdims=True)
    second = jnp.mean(grad * xhat, axis=-1, keepdims=True)
    return scale * (grad - first - xhat * second)


def total(x):
    return jnp.sum(x, axis=0, keepdims=True)


def sides():
    p = lax.axis_index("dom") % 2
    g = lax.axis_index("group") % 2
    return (p, 1 - p), (1 - p, p), (2 + g, 3 - g), (3 - g, 2 + g)


def write_sends(send_ref, rows, outs):
    for (src, _), out in zip(sides(), outs):
        picked = mm(pick_rows(send_ref[pl.ds(src, 1), :], 256), rows)
        out[...] = picked.astype(BF16)


def add_returns(send_ref, rets):
    out = jnp.zeros((256, H), F32)
    for (src, _), ret in zip(sides(), rets):
        out = out + mm(spread_rows(send_ref[pl.ds(src, 1), :], 256), ret[...])
    return out


def slot_rows(slot):
    return pl.ds(pl.multiple_of(256 + 128 * slot, 128), 128)


def fill_table(table, x_ref, got):
    table[0:256, :] = x_ref[...]
    for (_, dst), r in zip(sides(), got):
        table[slot_rows(dst), :] = r[...]


def write_backs(acc, outs):
    for (_, dst), out in zip(sides(), outs):
        out[...] = acc[slot_rows(dst), :].astype(BF16)


def fetch(pairs, sems):
    copies = [pltpu.make_async_copy(src, dst, sems.at[i]) for i, (src, dst) in enumerate(pairs)]
    for c in copies:
        c.start()
    return copies


def sends_kernel(send_hbm, x_hbm, o0, o1, o2, o3, send_ref, x_ref, sems):
    for c in fetch(((send_hbm, send_ref), (x_hbm, x_ref)), sems):
        c.wait()
    write_sends(send_ref, x_ref[...], (o0, o1, o2, o3))


def load_kernel(cnt_hbm, token, *refs):
    cnt_ref, sems = refs[-2:]
    n = len(refs) // 2 - 1
    copies = fetch(((cnt_hbm, cnt_ref), *zip(refs[:n], refs[n:-2])), sems)
    for c in copies:
        c.wait()
    snd_ref = refs[n]
    snd_ref[...] = slot_ids(snd_ref[...], [cnt_ref[0, k] for k in range(3)])


def edge_forward(snd_ref, rcv_ref, table, e_ref, w1, w2, b_ref, g_ref, joined, hidden, slope, xhat, scale, e_new, agg):
    agg[...] = jnp.zeros((256, H), F32)

    def step(i, carry):
        rows = pl.ds(pl.multiple_of(i * BLOCK, BLOCK), BLOCK)
        ids = snd_ref[i]
        sent = mm(pick_rows(ids, 768), table[...]).astype(BF16)
        recv = mm(pick_rows(rcv_ref[i], 256), table[0:256, :]).astype(BF16)
        joined[rows, 0:128] = e_ref[rows, :]
        joined[rows, 128:256] = sent
        joined[rows, 256:384] = recv
        pre = mm(joined[rows, :], w1[...]) + b_ref[0:1, :]
        act, slo = silu_parts(pre)
        act = act.astype(BF16)
        hidden[rows, :] = act
        slope[rows, :] = slo
        xh, sc = norm_parts(mm(act, w2[...]) + b_ref[1:2, :])
        xhat[rows, :] = xh
        scale[rows, :] = sc
        new = (e_ref[rows, :].astype(F32) + xh * g_ref[0:1, :]).astype(BF16)
        if e_new is not None:
            e_new[rows, :] = new
        agg[...] += mm(spread_rows(rcv_ref[i], 256), new)
        return carry

    lax.fori_loop(0, e_ref.shape[0] // BLOCK, step, 0, unroll=True)


def node_forward(x, agg, wn1, wn2, b_ref, g_ref):
    joined = jnp.concatenate([x, agg.astype(BF16)], axis=1)
    act, slo = silu_parts(mm(joined, wn1[...]) + b_ref[2:3, :])
    act = act.astype(BF16)
    xh, sc = norm_parts(mm(act, wn2[...]) + b_ref[3:4, :])
    new = (x.astype(F32) + xh * g_ref[1:2, :]).astype(BF16)
    return new, (joined, act, slo, xh, sc)


def node_backward(cot, saved, wn1, wn2, g_ref):
    joined, act, slo, xh, sc = saved
    cot = cot.astype(F32)
    back = norm_back(cot, xh, sc, g_ref[1:2, :])
    back_b = back.astype(BF16)
    dpre = mm_nt(back_b, wn2[...]).astype(BF16).astype(F32) * slo
    dpre_b = dpre.astype(BF16)
    djoined = mm_nt(dpre_b, wn1[...]).astype(BF16)
    small = (total(dpre), total(back), total(cot * xh))
    return cot + djoined[:, 0:128].astype(F32), djoined[:, 128:256], (joined, dpre_b, act, back_b), small


def edge_backward(snd_ref, rcv_ref, w1, w2, g_ref, slope, xhat, scale, dagg, e_cot, e_grad, acc, dpres, backs, sums):
    acc[...] = jnp.zeros(acc.shape, F32)
    sums[...] = jnp.zeros(sums.shape, F32)

    def step(i, carry):
        rows = pl.ds(pl.multiple_of(i * BLOCK, BLOCK), BLOCK)
        cot = mm(pick_rows(rcv_ref[i], 256), dagg)
        if e_cot is not None:
            cot = (cot + e_cot[rows, :].astype(F32)).astype(BF16).astype(F32)
        xh = xhat[rows, :]
        back = norm_back(cot, xh, scale[rows, :], g_ref[0:1, :])
        back_b = back.astype(BF16)
        dpre = mm_nt(back_b, w2[...]).astype(BF16).astype(F32) * slope[rows, :]
        dpre_b = dpre.astype(BF16)
        djoined = mm_nt(dpre_b, w1[...]).astype(BF16)
        e_grad[rows, :] = (cot + djoined[:, 0:128].astype(F32)).astype(BF16)
        acc[...] += mm(spread_rows(snd_ref[i], 768), djoined[:, 128:256])
        acc[0:256, :] += mm(spread_rows(rcv_ref[i], 256), djoined[:, 256:384])
        dpres[rows, :] = dpre_b
        backs[rows, :] = back_b
        sums[0:1, :] += total(dpre)
        sums[1:2, :] += total(back)
        sums[2:3, :] += total(cot * xh)
        return carry

    lax.fori_loop(0, slope.shape[0] // BLOCK, step, 0, unroll=True)


def weight_grads(node_ops, joined, dpres, hidden, backs, grads):
    joined_n, dpre_n, act_n, back_n = node_ops
    first = mm_tn(dpres[...], joined[...])
    for k in range(3):
        grads[128 * k : 128 * k + 128, :] = jnp.transpose(first[:, 128 * k : 128 * k + 128]).astype(BF16)
    grads[384:512, :] = jnp.transpose(mm_tn(backs[...], hidden[...])).astype(BF16)
    grads[512:768, :] = mm_tn(joined_n, dpre_n).astype(BF16)
    grads[768:896, :] = mm_tn(act_n, back_n).astype(BF16)


def grads_kernel(joined_n, dpre_n, act_n, back_n, joined, dpres, hidden, backs, tail, grads):
    weight_grads((joined_n[...], dpre_n[...], act_n[...], back_n[...]), joined, dpres, hidden, backs, grads)
    grads[896:GRAD_ROWS, :] = tail[...]


def small_rows(sums, small):
    tail = jnp.concatenate(
        [sums[0:2, :], small[0], small[1], sums[2:3, :], small[2], jnp.zeros((GRAD_ROWS - 902, H), F32)], axis=0
    )
    return tail.astype(BF16)


def first_kernel(
    snd_ref, rcv_ref, send_ref, x_ref, r0, r1, r2, r3, e_ref, w1, w2, wn1, wn2, b_ref, g_ref,
    joined, hidden, slope, xhat, scale, e_new, agg_b, x_new, o0, o1, o2, o3, table, agg,
):
    w1, w2, wn1, wn2, b_ref, g_ref = (r.at[0] for r in (w1, w2, wn1, wn2, b_ref, g_ref))
    fill_table(table, x_ref, (r0, r1, r2, r3))
    edge_forward(snd_ref, rcv_ref, table, e_ref, w1, w2, b_ref, g_ref, joined, hidden, slope, xhat, scale, e_new, agg)
    new, saved = node_forward(x_ref[...], agg[...], wn1, wn2, b_ref, g_ref)
    agg_b[...] = agg[...].astype(BF16)
    x_new[...] = new
    write_sends(send_ref, new, (o0, o1, o2, o3))


def last_kernel(
    snd_ref, rcv_ref, x_ref, r0, r1, r2, r3, e_ref, w1, w2, wn1, wn2, b_ref, g_ref, cot_ref,
    x_new, e_grad, x_grad, c0, c1, c2, c3, joined_n, dpre_n, act_n, back_n, joined, dpres, hidden, backs, tail,
    table, agg, slope, xhat, scale, acc, sums,
):
    w1, w2, wn1, wn2, b_ref, g_ref = (r.at[1] for r in (w1, w2, wn1, wn2, b_ref, g_ref))
    fill_table(table, x_ref, (r0, r1, r2, r3))
    edge_forward(snd_ref, rcv_ref, table, e_ref, w1, w2, b_ref, g_ref, joined, hidden, slope, xhat, scale, None, agg)
    new, saved = node_forward(x_ref[...], agg[...], wn1, wn2, b_ref, g_ref)
    x_new[...] = new
    dx, dagg, node_ops, small = node_backward(cot_ref[...], saved, wn1, wn2, g_ref)
    for out, op in zip((joined_n, dpre_n, act_n, back_n), node_ops):
        out[...] = op
    edge_backward(snd_ref, rcv_ref, w1, w2, g_ref, slope, xhat, scale, dagg, None, e_grad, acc, dpres, backs, sums)
    tail[...] = small_rows(sums, small)
    x_grad[...] = dx + acc[0:256, :]
    write_backs(acc, (c0, c1, c2, c3))


def back_kernel(
    snd_ref, rcv_ref, send_ref, x_ref, agg_b, own_ref, t0, t1, t2, t3, joined, hidden, slope, xhat, scale, e_cot, late,
    w1, w2, wn1, wn2, b_ref, g_ref,
    e_grad, x_grad, c0, c1, c2, c3, grads, acc, dpres, backs, sums,
):
    w1, w2, wn1, wn2, b_ref, g_ref = (r.at[0] for r in (w1, w2, wn1, wn2, b_ref, g_ref))
    grads[GRAD_ROWS:, :] = late[...]
    cot = (own_ref[...] + add_returns(send_ref, (t0, t1, t2, t3))).astype(BF16)
    new, saved = node_forward(x_ref[...], agg_b[...], wn1, wn2, b_ref, g_ref)
    dx, dagg, node_ops, small = node_backward(cot, saved, wn1, wn2, g_ref)
    edge_backward(snd_ref, rcv_ref, w1, w2, g_ref, slope, xhat, scale, dagg, e_cot, e_grad, acc, dpres, backs, sums)
    weight_grads(node_ops, joined, dpres, hidden, backs, grads)
    grads[896:GRAD_ROWS, :] = small_rows(sums, small)
    x_grad[...] = dx + acc[0:256, :]
    write_backs(acc, (c0, c1, c2, c3))


def finish_kernel(send_ref, own_ref, t0, t1, t2, t3, o_ref):
    o_ref[...] = (own_ref[...] + add_returns(send_ref, (t0, t1, t2, t3))).astype(BF16)


def shape(*dims, dtype=F32):
    return jax.ShapeDtypeStruct(dims, dtype)


SMEM = pltpu.SMEM
VMEM = pltpu.VMEM
HBM = pltpu.HBM


def call(kernel, outs, scratch, args, name, spaces=None, sems=0):
    spaces = spaces or [VMEM] * len(args)
    args = [pltpu.with_memory_space_constraint(a, m) if m is HBM else a for a, m in zip(args, spaces)]
    extra = [pltpu.SemaphoreType.DMA((sems,))] if sems else []
    return pl.pallas_call(
        kernel,
        out_shape=outs,
        in_specs=[pl.BlockSpec(memory_space=m) for m in spaces],
        out_specs=[pl.BlockSpec(memory_space=VMEM)] * len(outs),
        scratch_shapes=[s if s.__class__ is not jax.ShapeDtypeStruct else VMEM(s.shape, s.dtype) for s in scratch] + extra,
        compiler_params=pltpu.CompilerParams(vmem_limit_bytes=VMEM_LIMIT),
        name=name,
    )(*args)


def swaps(axis, first):
    size = lax.axis_size(axis)
    return [p for i in range(first, size - 1, 2) for p in ((i, i + 1), (i + 1, i))]


def exchange(blocks):
    plan = (("dom", 0), ("dom", 1), ("group", 0), ("group", 1))
    return [lax.ppermute(b, axis, swaps(axis, first)) for b, (axis, first) in zip(blocks, plan)]


def fold_kernel(x_ref, *refs):
    o_ref = refs[-1]
    out = jnp.sum(x_ref[...].astype(F32), axis=0).astype(BF16)
    for k in range(o_ref.shape[0]):
        o_ref[k] = out


def unpack_kernel(scale, x_ref, *outs):
    for out, (a, b) in zip(outs, CUTS):
        for l in range(2):
            out[l] = x_ref[GRAD_ROWS * l + a : GRAD_ROWS * l + b, :].astype(F32) * scale


def swap_tiles(x, axis):
    return lax.all_to_all(x, axis, split_axis=0, concat_axis=0, tiled=True)


def reduce_grads(packed, scale, first, second):
    dom, group = lax.axis_size("dom"), lax.axis_size("group")
    rows = packed.shape[0] // dom
    tiles = swap_tiles(packed.reshape(dom, rows, H), "dom")
    (tiles,) = call(fold_kernel, [shape(group, rows, H, dtype=BF16)], [], (tiles, *first), "fold_dom")
    tiles = swap_tiles(tiles, "group")
    (tiles,) = call(fold_kernel, [shape(dom, rows, H, dtype=BF16)], [], (tiles, *second), "fold_group")
    whole = swap_tiles(tiles, "dom").reshape(dom * rows, H)
    return call(partial(unpack_kernel, scale), [shape(2, b - a, H) for a, b in CUTS], [], (whole,), "unpack")


def shards(nodes, edges, node_cot, send_index, halo_count, senders, receivers, edge_in_w, edge_out_w, node_in_w, node_out_w, biases, gains):
    x0 = nodes[0]
    e0 = edges[0]
    send = send_index[0]
    n_edge = e0.shape[0]
    snd = senders[0].reshape(n_edge // BLOCK, 1, BLOCK)
    rcv = receivers[0].reshape(n_edge // BLOCK, 1, BLOCK)
    weights = (edge_in_w, edge_out_w, node_in_w, node_out_w, biases, gains)
    rows4 = [shape(H, H, dtype=BF16)] * 4
    residuals = [
        shape(n_edge, 3 * H, dtype=BF16),
        shape(n_edge, H, dtype=BF16),
        shape(n_edge, H),
        shape(n_edge, H),
        shape(n_edge, 1),
    ]
    low = shape(n_edge, H, dtype=BF16)
    small = shape(256, H, dtype=BF16)
    operands = [shape(256, 2 * H, dtype=BF16), small, small, small, residuals[0], low, low, low, shape(GRAD_ROWS - 896, H, dtype=BF16)]
    table = shape(768, H, dtype=BF16)

    *sent, send, x0 = call(
        sends_kernel,
        rows4 + [shape(4, H, dtype=jnp.int32), shape(256, H, dtype=BF16)],
        [],
        (send, x0),
        "sends",
        [HBM, HBM],
        2,
    )
    raw = (snd, rcv, e0, node_cot[0], *weights)
    loaded = call(
        load_kernel,
        [shape(*a.shape, dtype=a.dtype) for a in raw],
        [SMEM((1, 4), jnp.int32)],
        (halo_count, sent[0], *raw),
        "load",
        [HBM, VMEM] + [HBM] * len(raw),
        1 + len(raw),
    )
    snd, rcv, e0, cot, *weights = loaded
    got = exchange(sent)
    out = call(
        first_kernel,
        residuals + [shape(n_edge, H, dtype=BF16), shape(256, H, dtype=BF16), shape(256, H, dtype=BF16)] + rows4,
        [table, shape(256, H)],
        (snd, rcv, send, x0, *got, e0, *weights),
        "layer0",
    )
    saved, (e1, agg0, x1), sent = out[:5], out[5:8], out[8:]
    got = exchange(sent)
    out = call(
        last_kernel,
        [shape(256, H, dtype=BF16), shape(n_edge, H, dtype=BF16), shape(256, H)] + rows4 + operands,
        [table, shape(256, H)] + residuals[2:] + [shape(768, H), shape(8, H)],
        (snd, rcv, x1, *got, e1, *weights, cot),
        "layer1",
    )
    nodes_out, e_cot, own = out[:3]
    back = exchange(out[3:7])
    (grads1,) = call(grads_kernel, [shape(GRAD_ROWS, H, dtype=BF16)], [], out[7:], "wgrad1")
    out = call(
        back_kernel,
        [shape(n_edge, H, dtype=BF16), shape(256, H)] + rows4 + [shape(2 * GRAD_ROWS, H, dtype=BF16)],
        [shape(768, H), low, low, shape(8, H)],
        (snd, rcv, send, x0, agg0, own, *back, *saved, e_cot, grads1, *weights),
        "back0",
    )
    edge_grad, own = out[:2]
    packed = out[6]
    back = exchange(out[2:6])
    (node_grad,) = call(finish_kernel, [shape(256, H, dtype=BF16)], [], (send, own, *back), "finish")

    scale = (lax.axis_size("dom") * lax.axis_size("group") * x0.shape[0]) ** (-0.5)
    grads = reduce_grads(packed, scale, back[:2], ())
    return (nodes_out[None], node_grad[None], edge_grad[None], *grads)


def solution(mesh):
    part = ("dom", "group")
    in_specs = (P(part),) * 7 + (P(),) * 6
    out_specs = (P(part),) * 3 + (P(),) * 6
    return jax.shard_map(shards, mesh=mesh, in_specs=in_specs, out_specs=out_specs, check_vma=False)
```

```python
from functools import partial

import jax
import jax.numpy as jnp
from jax import lax
from jax.experimental import pallas as pl
from jax.experimental.pallas import tpu as pltpu
from jax.sharding import PartitionSpec as P

H = 128
BLOCK = 768
GRAD_ROWS = 1024
VMEM_LIMIT = 28 << 20
CUTS = ((0, 384), (384, 512), (512, 768), (768, 896), (896, 900), (900, 902))
F32 = jnp.float32
BF16 = jnp.bfloat16


def mm(a, b):
    return lax.dot_general(a, b, (((1,), (0,)), ((), ())), preferred_element_type=F32)


def mm_nt(a, b):
    return lax.dot_general(a, b, (((1,), (1,)), ((), ())), preferred_element_type=F32)


def mm_tn(a, b):
    return lax.dot_general(a, b, (((0,), (0,)), ((), ())), preferred_element_type=F32)


def column(row):
    return jnp.transpose(jnp.broadcast_to(row, (8, row.shape[1])))[:, :1]


def hot(mask):
    return jnp.where(mask, 1.0, 0.0).astype(BF16)


def pick_rows(row, width):
    col = column(row)
    return hot(lax.broadcasted_iota(jnp.int32, (row.shape[1], width), 1) == col)


def spread_rows(row, width):
    return hot(lax.broadcasted_iota(jnp.int32, (width, row.shape[1]), 0) == row)


def slot_ids(ids, counts):
    out = ids
    end = 256
    for k in range(3):
        end = end + counts[k]
        out = out + jnp.where(ids >= end, 128 - counts[k], 0)
    return out


def silu_parts(pre):
    sig = 0.5 * jnp.tanh(0.5 * pre) + 0.5
    return pre * sig, sig * (1.0 + pre * (1.0 - sig))


def norm_parts(mapped):
    centre = mapped - jnp.mean(mapped, axis=-1, keepdims=True)
    spread = jnp.mean(centre * centre, axis=-1, keepdims=True)
    scale = lax.rsqrt(spread + 1e-05)
    return centre * scale, scale


def norm_back(cot, xhat, scale, gain):
    grad = cot * gain
    first = jnp.mean(grad, axis=-1, keepdims=True)
    second = jnp.mean(grad * xhat, axis=-1, keepdims=True)
    return scale * (grad - first - xhat * second)


def total(x):
    return jnp.sum(x, axis=0, keepdims=True)


def sides():
    p = lax.axis_index("dom") % 2
    g = lax.axis_index("group") % 2
    return (p, 1 - p), (1 - p, p), (2 + g, 3 - g), (3 - g, 2 + g)


def write_sends(send_ref, rows, outs):
    for (src, _), out in zip(sides(), outs):
        picked = mm(pick_rows(send_ref[pl.ds(src, 1), :], 256), rows)
        out[...] = picked.astype(BF16)


def add_returns(send_ref, rets):
    out = jnp.zeros((256, H), F32)
    for (src, _), ret in zip(sides(), rets):
        out = out + mm(spread_rows(send_ref[pl.ds(src, 1), :], 256), ret[...])
    return out


def slot_rows(slot):
    return pl.ds(pl.multiple_of(256 + 128 * slot, 128), 128)


def fill_table(table, x_ref, got):
    table[0:256, :] = x_ref[...]
    for (_, dst), r in zip(sides(), got):
        table[slot_rows(dst), :] = r[...]


def write_backs(acc, outs):
    for (_, dst), out in zip(sides(), outs):
        out[...] = acc[slot_rows(dst), :].astype(BF16)


def fetch(pairs, sems):
    copies = [pltpu.make_async_copy(src, dst, sems.at[i]) for i, (src, dst) in enumerate(pairs)]
    for c in copies:
        c.start()
    return copies


def sends_kernel(send_hbm, x_hbm, o0, o1, o2, o3, send_ref, x_ref, sems):
    for c in fetch(((send_hbm, send_ref), (x_hbm, x_ref)), sems):
        c.wait()
    write_sends(send_ref, x_ref[...], (o0, o1, o2, o3))


def load_kernel(cnt_hbm, token, *refs):
    cnt_ref, sems = refs[-2:]
    n = len(refs) // 2 - 1
    copies = fetch(((cnt_hbm, cnt_ref), *zip(refs[:n], refs[n:-2])), sems)
    for c in copies:
        c.wait()
    snd_ref = refs[n]
    snd_ref[...] = slot_ids(snd_ref[...], [cnt_ref[0, k] for k in range(3)])


def edge_forward(snd_ref, rcv_ref, table, e_ref, w1, w2, b_ref, g_ref, joined, hidden, slope, xhat, scale, e_new, agg):
    def gather(i):
        rows = pl.ds(i * BLOCK, BLOCK)
        joined[rows, 0:128] = e_ref[rows, :]
        joined[rows, 128:256] = mm(pick_rows(snd_ref[i], 768), table[...]).astype(BF16)
        joined[rows, 256:384] = mm(pick_rows(rcv_ref[i], 256), table[0:256, :]).astype(BF16)

    def update(i):
        rows = pl.ds(i * BLOCK, BLOCK)
        act, slo = silu_parts(mm(joined[rows, :], w1[...]) + b_ref[0:1, :])
        act = act.astype(BF16)
        hidden[rows, :] = act
        slope[rows, :] = slo
        xh, sc = norm_parts(mm(act, w2[...]) + b_ref[1:2, :])
        xhat[rows, :] = xh
        scale[rows, :] = sc
        new = (e_ref[rows, :].astype(F32) + xh * g_ref[0:1, :]).astype(BF16)
        if e_new is not None:
            e_new[rows, :] = new
        return mm(spread_rows(rcv_ref[i], 256), new)

    blocks = e_ref.shape[0] // BLOCK
    gather(0)
    out = 0.0
    for i in range(blocks):
        if i + 1 < blocks:
            gather(i + 1)
        out = out + update(i)
    agg[...] = out


def node_forward(x, agg, wn1, wn2, b_ref, g_ref):
    joined = jnp.concatenate([x, agg.astype(BF16)], axis=1)
    act, slo = silu_parts(mm(joined, wn1[...]) + b_ref[2:3, :])
    act = act.astype(BF16)
    xh, sc = norm_parts(mm(act, wn2[...]) + b_ref[3:4, :])
    new = (x.astype(F32) + xh * g_ref[1:2, :]).astype(BF16)
    return new, (joined, act, slo, xh, sc)


def node_backward(cot, saved, wn1, wn2, g_ref):
    joined, act, slo, xh, sc = saved
    cot = cot.astype(F32)
    back = norm_back(cot, xh, sc, g_ref[1:2, :])
    back_b = back.astype(BF16)
    dpre = mm_nt(back_b, wn2[...]).astype(BF16).astype(F32) * slo
    dpre_b = dpre.astype(BF16)
    djoined = mm_nt(dpre_b, wn1[...]).astype(BF16)
    small = (total(dpre), total(back), total(cot * xh))
    return cot + djoined[:, 0:128].astype(F32), djoined[:, 128:256], (joined, dpre_b, act, back_b), small


def edge_backward(snd_ref, rcv_ref, w1, w2, g_ref, slope, xhat, scale, dagg, e_cot, e_grad, acc, dpres, backs, sums):
    acc[...] = jnp.zeros(acc.shape, F32)
    sums[...] = jnp.zeros(sums.shape, F32)

    def step(i, carry):
        rows = pl.ds(pl.multiple_of(i * BLOCK, BLOCK), BLOCK)
        cot = mm(pick_rows(rcv_ref[i], 256), dagg)
        if e_cot is not None:
            cot = (cot + e_cot[rows, :].astype(F32)).astype(BF16).astype(F32)
        xh = xhat[rows, :]
        back = norm_back(cot, xh, scale[rows, :], g_ref[0:1, :])
        back_b = back.astype(BF16)
        dpre = mm_nt(back_b, w2[...]).astype(BF16).astype(F32) * slope[rows, :]
        dpre_b = dpre.astype(BF16)
        djoined = mm_nt(dpre_b, w1[...]).astype(BF16)
        e_grad[rows, :] = (cot + djoined[:, 0:128].astype(F32)).astype(BF16)
        acc[...] += mm(spread_rows(snd_ref[i], 768), djoined[:, 128:256])
        acc[0:256, :] += mm(spread_rows(rcv_ref[i], 256), djoined[:, 256:384])
        dpres[rows, :] = dpre_b
        backs[rows, :] = back_b
        sums[0:1, :] += total(dpre)
        sums[1:2, :] += total(back)
        sums[2:3, :] += total(cot * xh)
        return carry

    lax.fori_loop(0, slope.shape[0] // BLOCK, step, 0, unroll=True)


def weight_grads(node_ops, joined, dpres, hidden, backs, grads):
    joined_n, dpre_n, act_n, back_n = node_ops
    first = mm_tn(dpres[...], joined[...])
    for k in range(3):
        grads[128 * k : 128 * k + 128, :] = jnp.transpose(first[:, 128 * k : 128 * k + 128]).astype(BF16)
    grads[384:512, :] = jnp.transpose(mm_tn(backs[...], hidden[...])).astype(BF16)
    grads[512:768, :] = mm_tn(joined_n, dpre_n).astype(BF16)
    grads[768:896, :] = mm_tn(act_n, back_n).astype(BF16)


def grads_kernel(joined_n, dpre_n, act_n, back_n, joined, dpres, hidden, backs, tail, grads):
    weight_grads((joined_n[...], dpre_n[...], act_n[...], back_n[...]), joined, dpres, hidden, backs, grads)
    grads[896:GRAD_ROWS, :] = tail[...]


def small_rows(sums, small):
    tail = jnp.concatenate(
        [sums[0:2, :], small[0], small[1], sums[2:3, :], small[2], jnp.zeros((GRAD_ROWS - 902, H), F32)], axis=0
    )
    return tail.astype(BF16)


def first_kernel(
    snd_ref, rcv_ref, send_ref, x_ref, r0, r1, r2, r3, e_ref, w1, w2, wn1, wn2, b_ref, g_ref,
    joined, hidden, slope, xhat, scale, e_new, agg_b, x_new, o0, o1, o2, o3, table, agg,
):
    w1, w2, wn1, wn2, b_ref, g_ref = (r.at[0] for r in (w1, w2, wn1, wn2, b_ref, g_ref))
    fill_table(table, x_ref, (r0, r1, r2, r3))
    edge_forward(snd_ref, rcv_ref, table, e_ref, w1, w2, b_ref, g_ref, joined, hidden, slope, xhat, scale, e_new, agg)
    new, saved = node_forward(x_ref[...], agg[...], wn1, wn2, b_ref, g_ref)
    agg_b[...] = agg[...].astype(BF16)
    x_new[...] = new
    write_sends(send_ref, new, (o0, o1, o2, o3))


def last_kernel(
    snd_ref, rcv_ref, x_ref, r0, r1, r2, r3, e_ref, w1, w2, wn1, wn2, b_ref, g_ref, cot_ref,
    x_new, e_grad, x_grad, c0, c1, c2, c3, joined_n, dpre_n, act_n, back_n, joined, dpres, hidden, backs, tail,
    table, agg, slope, xhat, scale, acc, sums,
):
    w1, w2, wn1, wn2, b_ref, g_ref = (r.at[1] for r in (w1, w2, wn1, wn2, b_ref, g_ref))
    fill_table(table, x_ref, (r0, r1, r2, r3))
    edge_forward(snd_ref, rcv_ref, table, e_ref, w1, w2, b_ref, g_ref, joined, hidden, slope, xhat, scale, None, agg)
    new, saved = node_forward(x_ref[...], agg[...], wn1, wn2, b_ref, g_ref)
    x_new[...] = new
    dx, dagg, node_ops, small = node_backward(cot_ref[...], saved, wn1, wn2, g_ref)
    for out, op in zip((joined_n, dpre_n, act_n, back_n), node_ops):
        out[...] = op
    edge_backward(snd_ref, rcv_ref, w1, w2, g_ref, slope, xhat, scale, dagg, None, e_grad, acc, dpres, backs, sums)
    tail[...] = small_rows(sums, small)
    x_grad[...] = dx + acc[0:256, :]
    write_backs(acc, (c0, c1, c2, c3))


def back_kernel(
    snd_ref, rcv_ref, send_ref, x_ref, agg_b, own_ref, t0, t1, t2, t3, joined, hidden, slope, xhat, scale, e_cot,
    w1, w2, wn1, wn2, b_ref, g_ref,
    e_grad, x_grad, c0, c1, c2, c3, grads, acc, dpres, backs, sums,
):
    w1, w2, wn1, wn2, b_ref, g_ref = (r.at[0] for r in (w1, w2, wn1, wn2, b_ref, g_ref))
    cot = (own_ref[...] + add_returns(send_ref, (t0, t1, t2, t3))).astype(BF16)
    new, saved = node_forward(x_ref[...], agg_b[...], wn1, wn2, b_ref, g_ref)
    dx, dagg, node_ops, small = node_backward(cot, saved, wn1, wn2, g_ref)
    edge_backward(snd_ref, rcv_ref, w1, w2, g_ref, slope, xhat, scale, dagg, e_cot, e_grad, acc, dpres, backs, sums)
    weight_grads(node_ops, joined, dpres, hidden, backs, grads)
    grads[896:GRAD_ROWS, :] = small_rows(sums, small)
    x_grad[...] = dx + acc[0:256, :]
    write_backs(acc, (c0, c1, c2, c3))


def finish_kernel(send_ref, own_ref, t0, t1, t2, t3, o_ref):
    o_ref[...] = (own_ref[...] + add_returns(send_ref, (t0, t1, t2, t3))).astype(BF16)


def shape(*dims, dtype=F32):
    return jax.ShapeDtypeStruct(dims, dtype)


SMEM = pltpu.SMEM
VMEM = pltpu.VMEM
HBM = pltpu.HBM


def call(kernel, outs, scratch, args, name, spaces=None, sems=0):
    spaces = spaces or [VMEM] * len(args)
    args = [pltpu.with_memory_space_constraint(a, m) if m is HBM else a for a, m in zip(args, spaces)]
    extra = [pltpu.SemaphoreType.DMA((sems,))] if sems else []
    return pl.pallas_call(
        kernel,
        out_shape=outs,
        in_specs=[pl.BlockSpec(memory_space=m) for m in spaces],
        out_specs=[pl.BlockSpec(memory_space=VMEM)] * len(outs),
        scratch_shapes=[s if s.__class__ is not jax.ShapeDtypeStruct else VMEM(s.shape, s.dtype) for s in scratch] + extra,
        compiler_params=pltpu.CompilerParams(vmem_limit_bytes=VMEM_LIMIT),
        name=name,
    )(*args)


def swaps(axis, first):
    size = lax.axis_size(axis)
    return [p for i in range(first, size - 1, 2) for p in ((i, i + 1), (i + 1, i))]


def exchange(blocks):
    plan = (("dom", 0), ("dom", 1), ("group", 0), ("group", 1))
    return [lax.ppermute(b, axis, swaps(axis, first)) for b, (axis, first) in zip(blocks, plan)]


def fold_kernel(x_ref, *refs):
    o_ref = refs[-1]
    out = jnp.sum(x_ref[...].astype(F32), axis=0).astype(BF16)
    for k in range(o_ref.shape[0]):
        o_ref[k] = out


def join_kernel(own0, own1, got1, got0, o_ref):
    core = lax.axis_index("dom") % 2

    @pl.when(core == 0)
    def _():
        o_ref[...] = (own0[...].astype(F32) + got0[...].astype(F32)).astype(BF16)

    @pl.when(core == 1)
    def _():
        o_ref[...] = (own1[...].astype(F32) + got1[...].astype(F32)).astype(BF16)


def unpack_kernel(scale, mine, other, *outs):
    core = lax.axis_index("dom") % 2
    for out, (a, b) in zip(outs, CUTS):
        out[core] = mine[a:b, :].astype(F32) * scale
        out[1 - core] = other[a:b, :].astype(F32) * scale


def on_chip(core):
    return [(i + core, i + 1 - core) for i in range(0, lax.axis_size("dom"), 2)]


def swap_tiles(x):
    dom, group = lax.axis_size("dom"), lax.axis_size("group")
    sets = [[d * group + g for d in range(c, dom, 2) for g in range(group)] for c in range(2)]
    return lax.all_to_all(x, ("dom", "group"), split_axis=0, concat_axis=0, axis_index_groups=sets, tiled=True)


def reduce_grads(grads0, grads1, early, scale, first, second):
    late = lax.ppermute(grads0, "dom", on_chip(1))
    (joined,) = call(join_kernel, [shape(GRAD_ROWS, H, dtype=BF16)], [], (grads0, grads1, early, late), "join")
    count = lax.axis_size("dom") * lax.axis_size("group") // 2
    tiles = swap_tiles(joined.reshape(count, -1, H))
    (tiles,) = call(fold_kernel, [shape(*tiles.shape, dtype=BF16)], [], (tiles, *first), "fold")
    mine, _ = lax.optimization_barrier((swap_tiles(tiles), second))
    mine = mine.reshape(GRAD_ROWS, H)
    other = lax.ppermute(mine, "dom", swaps("dom", 0))
    return call(partial(unpack_kernel, scale), [shape(2, b - a, H) for a, b in CUTS], [], (mine, other), "unpack")


def shards(nodes, edges, node_cot, send_index, halo_count, senders, receivers, edge_in_w, edge_out_w, node_in_w, node_out_w, biases, gains):
    x0 = nodes[0]
    e0 = edges[0]
    send = send_index[0]
    n_edge = e0.shape[0]
    snd = senders[0].reshape(n_edge // BLOCK, 1, BLOCK)
    rcv = receivers[0].reshape(n_edge // BLOCK, 1, BLOCK)
    weights = (edge_in_w, edge_out_w, node_in_w, node_out_w, biases, gains)
    rows4 = [shape(H, H, dtype=BF16)] * 4
    residuals = [
        shape(n_edge, 3 * H, dtype=BF16),
        shape(n_edge, H, dtype=BF16),
        shape(n_edge, H),
        shape(n_edge, H),
        shape(n_edge, 1),
    ]
    low = shape(n_edge, H, dtype=BF16)
    small = shape(256, H, dtype=BF16)
    operands = [shape(256, 2 * H, dtype=BF16), small, small, small, residuals[0], low, low, low, shape(GRAD_ROWS - 896, H, dtype=BF16)]
    table = shape(768, H, dtype=BF16)

    *sent, send, x0 = call(
        sends_kernel,
        rows4 + [shape(4, H, dtype=jnp.int32), shape(256, H, dtype=BF16)],
        [],
        (send, x0),
        "sends",
        [HBM, HBM],
        2,
    )
    raw = (snd, rcv, e0, node_cot[0], *weights)
    loaded = call(
        load_kernel,
        [shape(*a.shape, dtype=a.dtype) for a in raw],
        [SMEM((1, 4), jnp.int32)],
        (halo_count, sent[0], *raw),
        "load",
        [HBM, VMEM] + [HBM] * len(raw),
        1 + len(raw),
    )
    snd, rcv, e0, cot, *weights = loaded
    got = exchange(sent)
    out = call(
        first_kernel,
        residuals + [shape(n_edge, H, dtype=BF16), shape(256, H, dtype=BF16), shape(256, H, dtype=BF16)] + rows4,
        [table, shape(256, H)],
        (snd, rcv, send, x0, *got, e0, *weights),
        "layer0",
    )
    saved, (e1, agg0, x1), sent = out[:5], out[5:8], out[8:]
    got = exchange(sent)
    out = call(
        last_kernel,
        [shape(256, H, dtype=BF16), shape(n_edge, H, dtype=BF16), shape(256, H)] + rows4 + operands,
        [table, shape(256, H)] + residuals[2:] + [shape(768, H), shape(8, H)],
        (snd, rcv, x1, *got, e1, *weights, cot),
        "layer1",
    )
    nodes_out, e_cot, own = out[:3]
    back = exchange(out[3:7])
    (grads1,) = call(grads_kernel, [shape(GRAD_ROWS, H, dtype=BF16)], [], out[7:], "wgrad1")
    early = lax.ppermute(grads1, "dom", on_chip(0))
    out = call(
        back_kernel,
        [shape(n_edge, H, dtype=BF16), shape(256, H)] + rows4 + [shape(GRAD_ROWS, H, dtype=BF16)],
        [shape(768, H), low, low, shape(8, H)],
        (snd, rcv, send, x0, agg0, own, *back, *saved, e_cot, *weights),
        "back0",
    )
    edge_grad, own = out[:2]
    grads0 = out[6]
    back = exchange(out[2:6])
    (node_grad,) = call(finish_kernel, [shape(256, H, dtype=BF16)], [], (send, own, *back), "finish")

    scale = (lax.axis_size("dom") * lax.axis_size("group") * x0.shape[0]) ** (-0.5)
    grads = reduce_grads(grads0, grads1, early, scale, back[:2], back[2:])
    return (nodes_out[None], node_grad[None], edge_grad[None], *grads)


def solution(mesh):
    part = ("dom", "group")
    in_specs = (P(part),) * 7 + (P(),) * 6
    out_specs = (P(part),) * 3 + (P(),) * 6
    return jax.shard_map(shards, mesh=mesh, in_specs=in_specs, out_specs=out_specs, check_vma=False)
```

```python
from functools import partial

import jax
import jax.numpy as jnp
from jax import lax
from jax.experimental import pallas as pl
from jax.experimental.pallas import tpu as pltpu
from jax.sharding import PartitionSpec as P

H = 128
BLOCK = 768
GRAD_ROWS = 1024
VMEM_LIMIT = 28 << 20
CUTS = ((0, 384), (384, 512), (512, 768), (768, 896), (896, 900), (900, 902))
F32 = jnp.float32
BF16 = jnp.bfloat16


def mm(a, b):
    return lax.dot_general(a, b, (((1,), (0,)), ((), ())), preferred_element_type=F32)


def mm_nt(a, b):
    return lax.dot_general(a, b, (((1,), (1,)), ((), ())), preferred_element_type=F32)


def mm_tn(a, b):
    return lax.dot_general(a, b, (((0,), (0,)), ((), ())), preferred_element_type=F32)


def column(row):
    return jnp.transpose(jnp.broadcast_to(row, (8, row.shape[1])))[:, :1]


def hot(mask):
    return jnp.where(mask, 1.0, 0.0).astype(BF16)


def pick_rows(row, width):
    col = column(row)
    return hot(lax.broadcasted_iota(jnp.int32, (row.shape[1], width), 1) == col)


def spread_rows(row, width):
    return hot(lax.broadcasted_iota(jnp.int32, (width, row.shape[1]), 0) == row)


def slot_ids(ids, counts):
    out = ids
    end = 256
    for k in range(3):
        end = end + counts[k]
        out = out + jnp.where(ids >= end, 128 - counts[k], 0)
    return out


def silu_parts(pre):
    sig = 0.5 * jnp.tanh(0.5 * pre) + 0.5
    return pre * sig, sig * (1.0 + pre * (1.0 - sig))


def norm_parts(mapped):
    centre = mapped - jnp.mean(mapped, axis=-1, keepdims=True)
    spread = jnp.mean(centre * centre, axis=-1, keepdims=True)
    scale = lax.rsqrt(spread + 1e-05)
    return centre * scale, scale


def norm_back(cot, xhat, scale, gain):
    grad = cot * gain
    first = jnp.mean(grad, axis=-1, keepdims=True)
    second = jnp.mean(grad * xhat, axis=-1, keepdims=True)
    return scale * (grad - first - xhat * second)


def total(x):
    return jnp.sum(x, axis=0, keepdims=True)


def sides():
    p = lax.axis_index("dom") % 2
    g = lax.axis_index("group") % 2
    return (p, 1 - p), (1 - p, p), (2 + g, 3 - g), (3 - g, 2 + g)


def write_sends(send_ref, rows, outs):
    for (src, _), out in zip(sides(), outs):
        picked = mm(pick_rows(send_ref[pl.ds(src, 1), :], 256), rows)
        out[...] = picked.astype(BF16)


def add_returns(send_ref, rets):
    out = jnp.zeros((256, H), F32)
    for (src, _), ret in zip(sides(), rets):
        out = out + mm(spread_rows(send_ref[pl.ds(src, 1), :], 256), ret[...])
    return out


def slot_rows(slot):
    return pl.ds(pl.multiple_of(256 + 128 * slot, 128), 128)


def fill_table(table, x_ref, got):
    table[0:256, :] = x_ref[...]
    for (_, dst), r in zip(sides(), got):
        table[slot_rows(dst), :] = r[...]


def write_backs(acc, outs):
    for (_, dst), out in zip(sides(), outs):
        out[...] = acc[slot_rows(dst), :].astype(BF16)


def fetch(pairs, sems):
    copies = [pltpu.make_async_copy(src, dst, sems.at[i]) for i, (src, dst) in enumerate(pairs)]
    for c in copies:
        c.start()
    return copies


def sends_kernel(send_hbm, x_hbm, o0, o1, o2, o3, send_ref, x_ref, sems):
    for c in fetch(((send_hbm, send_ref), (x_hbm, x_ref)), sems):
        c.wait()
    write_sends(send_ref, x_ref[...], (o0, o1, o2, o3))


def load_kernel(cnt_hbm, token, *refs):
    cnt_ref, sems = refs[-2:]
    n = len(refs) // 2 - 1
    copies = fetch(((cnt_hbm, cnt_ref), *zip(refs[:n], refs[n:-2])), sems)
    for c in copies:
        c.wait()
    snd_ref = refs[n]
    snd_ref[...] = slot_ids(snd_ref[...], [cnt_ref[0, k] for k in range(3)])


def gather_own(i, snd_ref, rcv_ref, x_ref, e_ref, joined):
    rows = pl.ds(i * BLOCK, BLOCK)
    joined[rows, 0:128] = e_ref[rows, :]
    joined[rows, 128:256] = mm(pick_rows(snd_ref[i], 256), x_ref[0:256, :]).astype(BF16)
    joined[rows, 256:384] = mm(pick_rows(rcv_ref[i], 256), x_ref[0:256, :]).astype(BF16)


def edge_forward(gather, pre_of, rcv_ref, e_ref, w2, b_ref, g_ref, hidden, slope, xhat, scale, e_new, agg):
    def update(i):
        rows = pl.ds(i * BLOCK, BLOCK)
        act, slo = silu_parts(pre_of(rows))
        act = act.astype(BF16)
        hidden[rows, :] = act
        slope[rows, :] = slo
        xh, sc = norm_parts(mm(act, w2[...]) + b_ref[1:2, :])
        xhat[rows, :] = xh
        scale[rows, :] = sc
        new = (e_ref[rows, 0:128].astype(F32) + xh * g_ref[0:1, :]).astype(BF16)
        if e_new is not None:
            e_new[rows, :] = new
        return mm(spread_rows(rcv_ref[i], 256), new)

    blocks = e_ref.shape[0] // BLOCK
    gather(0)
    out = 0.0
    for i in range(blocks):
        if i + 1 < blocks:
            gather(i + 1)
        out = out + update(i)
    agg[...] = out


def node_forward(x, agg, wn1, wn2, b_ref, g_ref):
    joined = jnp.concatenate([x, agg.astype(BF16)], axis=1)
    act, slo = silu_parts(mm(joined, wn1[...]) + b_ref[2:3, :])
    act = act.astype(BF16)
    xh, sc = norm_parts(mm(act, wn2[...]) + b_ref[3:4, :])
    new = (x.astype(F32) + xh * g_ref[1:2, :]).astype(BF16)
    return new, (joined, act, slo, xh, sc)


def node_backward(cot, saved, wn1, wn2, g_ref):
    joined, act, slo, xh, sc = saved
    cot = cot.astype(F32)
    back = norm_back(cot, xh, sc, g_ref[1:2, :])
    back_b = back.astype(BF16)
    dpre = mm_nt(back_b, wn2[...]).astype(BF16).astype(F32) * slo
    dpre_b = dpre.astype(BF16)
    djoined = mm_nt(dpre_b, wn1[...]).astype(BF16)
    small = (total(dpre), total(back), total(cot * xh))
    return cot + djoined[:, 0:128].astype(F32), djoined[:, 128:256], (joined, dpre_b, act, back_b), small


def edge_backward(snd_ref, rcv_ref, w1, w2, g_ref, slope, xhat, scale, dagg, e_cot, e_grad, acc, dpres, backs, sums):
    acc[...] = jnp.zeros(acc.shape, F32)
    sums[...] = jnp.zeros(sums.shape, F32)

    def step(i, carry):
        rows = pl.ds(pl.multiple_of(i * BLOCK, BLOCK), BLOCK)
        cot = mm(pick_rows(rcv_ref[i], 256), dagg)
        if e_cot is not None:
            cot = (cot + e_cot[rows, :].astype(F32)).astype(BF16).astype(F32)
        xh = xhat[rows, :]
        back = norm_back(cot, xh, scale[rows, :], g_ref[0:1, :])
        back_b = back.astype(BF16)
        dpre = mm_nt(back_b, w2[...]).astype(BF16).astype(F32) * slope[rows, :]
        dpre_b = dpre.astype(BF16)
        djoined = mm_nt(dpre_b, w1[...]).astype(BF16)
        e_grad[rows, :] = (cot + djoined[:, 0:128].astype(F32)).astype(BF16)
        acc[...] += mm(spread_rows(snd_ref[i], 768), djoined[:, 128:256])
        acc[0:256, :] += mm(spread_rows(rcv_ref[i], 256), djoined[:, 256:384])
        dpres[rows, :] = dpre_b
        backs[rows, :] = back_b
        sums[0:1, :] += total(dpre)
        sums[1:2, :] += total(back)
        sums[2:3, :] += total(cot * xh)
        return carry

    lax.fori_loop(0, slope.shape[0] // BLOCK, step, 0, unroll=True)


def weight_grads(node_ops, joined, dpres, hidden, backs, grads):
    joined_n, dpre_n, act_n, back_n = node_ops
    first = mm_tn(dpres[...], joined[...])
    for k in range(3):
        grads[128 * k : 128 * k + 128, :] = jnp.transpose(first[:, 128 * k : 128 * k + 128]).astype(BF16)
    grads[384:512, :] = jnp.transpose(mm_tn(backs[...], hidden[...])).astype(BF16)
    grads[512:768, :] = mm_tn(joined_n, dpre_n).astype(BF16)
    grads[768:896, :] = mm_tn(act_n, back_n).astype(BF16)


def own_kernel(snd_ref, rcv_ref, x_ref, e_ref, w1, b_ref, joined, pre_own):
    for i in range(e_ref.shape[0] // BLOCK):
        rows = pl.ds(i * BLOCK, BLOCK)
        gather_own(i, snd_ref, rcv_ref, x_ref, e_ref, joined)
        pre_own[rows, :] = mm(joined[rows, :], w1[1]) + b_ref[1, 0:1, :]


def grads_kernel(
    joined_n, dpre_n, act_n, back_n, halo, dpres, hidden, backs, tail, joined, x_ref, agg_b, wn1, wn2, b_ref, g_ref,
    grads, *node_saved,
):
    first = joined[...]
    first = jnp.concatenate([first[:, 0:128], first[:, 128:256] + halo[...], first[:, 256:384]], axis=1)
    weight_grads((joined_n[...], dpre_n[...], act_n[...], back_n[...]), first, dpres, hidden, backs, grads)
    grads[896:GRAD_ROWS, :] = tail[...]
    _, saved = node_forward(x_ref[...], agg_b[...], wn1.at[0], wn2.at[0], b_ref.at[0], g_ref.at[0])
    for out, value in zip(node_saved, saved):
        out[...] = value


def small_rows(sums, small):
    tail = jnp.concatenate(
        [sums[0:2, :], small[0], small[1], sums[2:3, :], small[2], jnp.zeros((GRAD_ROWS - 902, H), F32)], axis=0
    )
    return tail.astype(BF16)


def first_kernel(
    snd_ref, rcv_ref, send_ref, x_ref, r0, r1, r2, r3, e_ref, w1, w2, wn1, wn2, b_ref, g_ref,
    joined, hidden, slope, xhat, scale, e_new, agg_b, x_new, o0, o1, o2, o3, table, agg,
):
    w1, w2, wn1, wn2, b_ref, g_ref = (r.at[0] for r in (w1, w2, wn1, wn2, b_ref, g_ref))
    fill_table(table, x_ref, (r0, r1, r2, r3))

    def gather(i):
        rows = pl.ds(i * BLOCK, BLOCK)
        joined[rows, 0:128] = e_ref[rows, :]
        joined[rows, 128:256] = mm(pick_rows(snd_ref[i], 768), table[...]).astype(BF16)
        joined[rows, 256:384] = mm(pick_rows(rcv_ref[i], 256), table[0:256, :]).astype(BF16)

    def pre_of(rows):
        return mm(joined[rows, :], w1[...]) + b_ref[0:1, :]

    edge_forward(gather, pre_of, rcv_ref, e_ref, w2, b_ref, g_ref, hidden, slope, xhat, scale, e_new, agg)
    new, saved = node_forward(x_ref[...], agg[...], wn1, wn2, b_ref, g_ref)
    agg_b[...] = agg[...].astype(BF16)
    x_new[...] = new
    write_sends(send_ref, new, (o0, o1, o2, o3))


def last_kernel(
    snd_ref, rcv_ref, x_ref, r0, r1, r2, r3, joined, pre_own, w1, w2, wn1, wn2, b_ref, g_ref, cot_ref,
    x_new, e_grad, x_grad, c0, c1, c2, c3, joined_n, dpre_n, act_n, back_n, halo, dpres, hidden, backs, tail,
    table, agg, slope, xhat, scale, acc, sums,
):
    w1, w2, wn1, wn2, b_ref, g_ref = (r.at[1] for r in (w1, w2, wn1, wn2, b_ref, g_ref))
    fill_table(table, x_ref, (r0, r1, r2, r3))

    def gather(i):
        picked = mm(pick_rows(snd_ref[i] - 256, 512), table[256:768, :])
        halo[pl.ds(i * BLOCK, BLOCK), :] = picked.astype(BF16)

    def pre_of(rows):
        return pre_own[rows, :] + mm(halo[rows, :], w1[128:256, :])

    edge_forward(gather, pre_of, rcv_ref, joined, w2, b_ref, g_ref, hidden, slope, xhat, scale, None, agg)
    new, saved = node_forward(x_ref[...], agg[...], wn1, wn2, b_ref, g_ref)
    x_new[...] = new
    dx, dagg, node_ops, small = node_backward(cot_ref[...], saved, wn1, wn2, g_ref)
    for out, op in zip((joined_n, dpre_n, act_n, back_n), node_ops):
        out[...] = op
    edge_backward(snd_ref, rcv_ref, w1, w2, g_ref, slope, xhat, scale, dagg, None, e_grad, acc, dpres, backs, sums)
    tail[...] = small_rows(sums, small)
    x_grad[...] = dx + acc[0:256, :]
    write_backs(acc, (c0, c1, c2, c3))


def back_kernel(
    snd_ref, rcv_ref, send_ref, n0, n1, n2, n3, n4, own_ref, t0, t1, t2, t3, joined, hidden, slope, xhat, scale, e_cot, late,
    w1, w2, wn1, wn2, b_ref, g_ref,
    e_grad, x_grad, c0, c1, c2, c3, grads, acc, dpres, backs, sums,
):
    w1, w2, wn1, wn2, b_ref, g_ref = (r.at[0] for r in (w1, w2, wn1, wn2, b_ref, g_ref))
    grads[GRAD_ROWS:, :] = late[...]
    cot = (own_ref[...] + add_returns(send_ref, (t0, t1, t2, t3))).astype(BF16)
    saved = tuple(r[...] for r in (n0, n1, n2, n3, n4))
    dx, dagg, node_ops, small = node_backward(cot, saved, wn1, wn2, g_ref)
    edge_backward(snd_ref, rcv_ref, w1, w2, g_ref, slope, xhat, scale, dagg, e_cot, e_grad, acc, dpres, backs, sums)
    weight_grads(node_ops, joined, dpres, hidden, backs, grads)
    grads[896:GRAD_ROWS, :] = small_rows(sums, small)
    x_grad[...] = dx + acc[0:256, :]
    write_backs(acc, (c0, c1, c2, c3))


def finish_kernel(send_ref, own_ref, t0, t1, t2, t3, o_ref):
    o_ref[...] = (own_ref[...] + add_returns(send_ref, (t0, t1, t2, t3))).astype(BF16)


def shape(*dims, dtype=F32):
    return jax.ShapeDtypeStruct(dims, dtype)


SMEM = pltpu.SMEM
VMEM = pltpu.VMEM
HBM = pltpu.HBM


def call(kernel, outs, scratch, args, name, spaces=None, sems=0):
    spaces = spaces or [VMEM] * len(args)
    args = [pltpu.with_memory_space_constraint(a, m) if m is HBM else a for a, m in zip(args, spaces)]
    extra = [pltpu.SemaphoreType.DMA((sems,))] if sems else []
    return pl.pallas_call(
        kernel,
        out_shape=outs,
        in_specs=[pl.BlockSpec(memory_space=m) for m in spaces],
        out_specs=[pl.BlockSpec(memory_space=VMEM)] * len(outs),
        scratch_shapes=[s if s.__class__ is not jax.ShapeDtypeStruct else VMEM(s.shape, s.dtype) for s in scratch] + extra,
        compiler_params=pltpu.CompilerParams(vmem_limit_bytes=VMEM_LIMIT),
        name=name,
    )(*args)


def swaps(axis, first):
    size = lax.axis_size(axis)
    return [p for i in range(first, size - 1, 2) for p in ((i, i + 1), (i + 1, i))]


def exchange(blocks):
    plan = (("dom", 0), ("dom", 1), ("group", 0), ("group", 1))
    return [lax.ppermute(b, axis, swaps(axis, first)) for b, (axis, first) in zip(blocks, plan)]


def fold_kernel(x_ref, *refs):
    o_ref = refs[-1]
    out = jnp.sum(x_ref[...].astype(F32), axis=0).astype(BF16)
    for k in range(o_ref.shape[0]):
        o_ref[k] = out


def unpack_kernel(scale, x_ref, *outs):
    for out, (a, b) in zip(outs, CUTS):
        for l in range(2):
            out[l] = x_ref[GRAD_ROWS * l + a : GRAD_ROWS * l + b, :].astype(F32) * scale


def swap_tiles(x, axis):
    return lax.all_to_all(x, axis, split_axis=0, concat_axis=0, tiled=True)


def reduce_grads(packed, scale, first, second):
    dom, group = lax.axis_size("dom"), lax.axis_size("group")
    rows = packed.shape[0] // dom
    tiles = swap_tiles(packed.reshape(dom, rows, H), "dom")
    (tiles,) = call(fold_kernel, [shape(group, rows, H, dtype=BF16)], [], (tiles, *first), "fold_dom")
    tiles = swap_tiles(tiles, "group")
    (tiles,) = call(fold_kernel, [shape(dom, rows, H, dtype=BF16)], [], (tiles, *second), "fold_group")
    whole = swap_tiles(tiles, "dom").reshape(dom * rows, H)
    return call(partial(unpack_kernel, scale), [shape(2, b - a, H) for a, b in CUTS], [], (whole,), "unpack")


def shards(nodes, edges, node_cot, send_index, halo_count, senders, receivers, edge_in_w, edge_out_w, node_in_w, node_out_w, biases, gains):
    x0 = nodes[0]
    e0 = edges[0]
    send = send_index[0]
    n_edge = e0.shape[0]
    snd = senders[0].reshape(n_edge // BLOCK, 1, BLOCK)
    rcv = receivers[0].reshape(n_edge // BLOCK, 1, BLOCK)
    weights = (edge_in_w, edge_out_w, node_in_w, node_out_w, biases, gains)
    rows4 = [shape(H, H, dtype=BF16)] * 4
    residuals = [
        shape(n_edge, 3 * H, dtype=BF16),
        shape(n_edge, H, dtype=BF16),
        shape(n_edge, H),
        shape(n_edge, H),
        shape(n_edge, 1),
    ]
    low = shape(n_edge, H, dtype=BF16)
    small = shape(256, H, dtype=BF16)
    operands = [shape(256, 2 * H, dtype=BF16), small, small, small, low, low, low, low, shape(GRAD_ROWS - 896, H, dtype=BF16)]
    table = shape(768, H, dtype=BF16)

    *sent, send, x0 = call(
        sends_kernel,
        rows4 + [shape(4, H, dtype=jnp.int32), shape(256, H, dtype=BF16)],
        [],
        (send, x0),
        "sends",
        [HBM, HBM],
        2,
    )
    raw = (snd, rcv, e0, node_cot[0], *weights)
    loaded = call(
        load_kernel,
        [shape(*a.shape, dtype=a.dtype) for a in raw],
        [SMEM((1, 4), jnp.int32)],
        (halo_count, sent[0], *raw),
        "load",
        [HBM, VMEM] + [HBM] * len(raw),
        1 + len(raw),
    )
    snd, rcv, e0, cot, *weights = loaded
    got = exchange(sent)
    out = call(
        first_kernel,
        residuals + [shape(n_edge, H, dtype=BF16), shape(256, H, dtype=BF16), shape(256, H, dtype=BF16)] + rows4,
        [table, shape(256, H)],
        (snd, rcv, send, x0, *got, e0, *weights),
        "layer0",
    )
    saved, (e1, agg0, x1), sent = out[:5], out[5:8], out[8:]
    got = exchange(sent)
    joined1, pre1 = call(
        own_kernel,
        [residuals[0], shape(n_edge, H)],
        [],
        (snd, rcv, x1, e1, weights[0], weights[4]),
        "own1",
    )
    out = call(
        last_kernel,
        [shape(256, H, dtype=BF16), shape(n_edge, H, dtype=BF16), shape(256, H)] + rows4 + operands,
        [table, shape(256, H)] + residuals[2:] + [shape(768, H), shape(8, H)],
        (snd, rcv, x1, *got, joined1, pre1, *weights, cot),
        "layer1",
    )
    nodes_out, e_cot, own = out[:3]
    back = exchange(out[3:7])
    grads1, *node0 = call(
        grads_kernel,
        [shape(GRAD_ROWS, H, dtype=BF16), shape(256, 2 * H, dtype=BF16), small, shape(256, H), shape(256, H), shape(256, 1)],
        [],
        (*out[7:], joined1, x0, agg0, *weights[2:]),
        "wgrad1",
    )
    out = call(
        back_kernel,
        [shape(n_edge, H, dtype=BF16), shape(256, H)] + rows4 + [shape(2 * GRAD_ROWS, H, dtype=BF16)],
        [shape(768, H), low, low, shape(8, H)],
        (snd, rcv, send, *node0, own, *back, *saved, e_cot, grads1, *weights),
        "back0",
    )
    edge_grad, own = out[:2]
    packed = out[6]
    back = exchange(out[2:6])
    (node_grad,) = call(finish_kernel, [shape(256, H, dtype=BF16)], [], (send, own, *back), "finish")

    scale = (lax.axis_size("dom") * lax.axis_size("group") * x0.shape[0]) ** (-0.5)
    grads = reduce_grads(packed, scale, back[:2], ())
    return (nodes_out[None], node_grad[None], edge_grad[None], *grads)


def solution(mesh):
    part = ("dom", "group")
    in_specs = (P(part),) * 7 + (P(),) * 6
    out_specs = (P(part),) * 3 + (P(),) * 6
    return jax.shard_map(shards, mesh=mesh, in_specs=in_specs, out_specs=out_specs, check_vma=False)
```

```python
from functools import partial

import jax
import jax.numpy as jnp
from jax import lax
from jax.experimental import pallas as pl
from jax.experimental.pallas import tpu as pltpu
from jax.sharding import PartitionSpec as P

H = 128
BLOCK = 768
GRAD_ROWS = 1024
VMEM_LIMIT = 28 << 20
CUTS = ((0, 384), (384, 512), (512, 768), (768, 896), (896, 900), (900, 902))
F32 = jnp.float32
BF16 = jnp.bfloat16


def mm(a, b):
    return lax.dot_general(a, b, (((1,), (0,)), ((), ())), preferred_element_type=F32)


def mm_nt(a, b):
    return lax.dot_general(a, b, (((1,), (1,)), ((), ())), preferred_element_type=F32)


def mm_tn(a, b):
    return lax.dot_general(a, b, (((0,), (0,)), ((), ())), preferred_element_type=F32)


def column(row):
    return jnp.transpose(jnp.broadcast_to(row, (8, row.shape[1])))[:, :1]


def hot(mask):
    return jnp.where(mask, 1.0, 0.0).astype(BF16)


def pick_rows(row, width):
    col = column(row)
    return hot(lax.broadcasted_iota(jnp.int32, (row.shape[1], width), 1) == col)


def spread_rows(row, width):
    return hot(lax.broadcasted_iota(jnp.int32, (width, row.shape[1]), 0) == row)


def slot_ids(ids, counts):
    out = ids
    end = 256
    for k in range(3):
        end = end + counts[k]
        out = out + jnp.where(ids >= end, 128 - counts[k], 0)
    return out


def silu_parts(pre):
    sig = 0.5 * jnp.tanh(0.5 * pre) + 0.5
    return pre * sig, sig * (1.0 + pre * (1.0 - sig))


def norm_parts(mapped):
    centre = mapped - jnp.mean(mapped, axis=-1, keepdims=True)
    spread = jnp.mean(centre * centre, axis=-1, keepdims=True)
    scale = lax.rsqrt(spread + 1e-05)
    return centre * scale, scale


def norm_back(cot, xhat, scale, gain):
    grad = cot * gain
    first = jnp.mean(grad, axis=-1, keepdims=True)
    second = jnp.mean(grad * xhat, axis=-1, keepdims=True)
    return scale * (grad - first - xhat * second)


def total(x):
    return jnp.sum(x, axis=0, keepdims=True)


def sides():
    p = lax.axis_index("dom") % 2
    g = lax.axis_index("group") % 2
    return (p, 1 - p), (1 - p, p), (2 + g, 3 - g), (3 - g, 2 + g)


def write_sends(send_ref, rows, outs):
    for (src, _), out in zip(sides(), outs):
        picked = mm(pick_rows(send_ref[pl.ds(src, 1), :], 256), rows)
        out[...] = picked.astype(BF16)


def add_returns(send_ref, rets):
    out = jnp.zeros((256, H), F32)
    for (src, _), ret in zip(sides(), rets):
        out = out + mm(spread_rows(send_ref[pl.ds(src, 1), :], 256), ret[...])
    return out


def slot_rows(slot):
    return pl.ds(pl.multiple_of(256 + 128 * slot, 128), 128)


def fill_table(table, x_ref, got):
    table[0:256, :] = x_ref[...]
    for (_, dst), r in zip(sides(), got):
        table[slot_rows(dst), :] = r[...]


def write_backs(acc, outs):
    for (_, dst), out in zip(sides(), outs):
        out[...] = acc[slot_rows(dst), :].astype(BF16)


def fetch(pairs, sems):
    copies = [pltpu.make_async_copy(src, dst, sems.at[i]) for i, (src, dst) in enumerate(pairs)]
    for c in copies:
        c.start()
    return copies


def sends_kernel(send_hbm, x_hbm, o0, o1, o2, o3, send_ref, x_ref, sems):
    for c in fetch(((send_hbm, send_ref), (x_hbm, x_ref)), sems):
        c.wait()
    write_sends(send_ref, x_ref[...], (o0, o1, o2, o3))


def load_kernel(cnt_hbm, token, *refs):
    cnt_ref, sems = refs[-2:]
    n = len(refs) // 2 - 1
    copies = fetch(((cnt_hbm, cnt_ref), *zip(refs[:n], refs[n:-2])), sems)
    for c in copies:
        c.wait()
    snd_ref = refs[n]
    snd_ref[...] = slot_ids(snd_ref[...], [cnt_ref[0, k] for k in range(3)])


def gather_own(i, snd_ref, rcv_ref, x_ref, e_ref, joined):
    rows = pl.ds(i * BLOCK, BLOCK)
    joined[rows, 0:128] = e_ref[rows, :]
    joined[rows, 128:256] = mm(pick_rows(snd_ref[i], 256), x_ref[0:256, :]).astype(BF16)
    joined[rows, 256:384] = mm(pick_rows(rcv_ref[i], 256), x_ref[0:256, :]).astype(BF16)


def edge_forward(gather, pre_of, rcv_ref, e_ref, w2, b_ref, g_ref, hidden, slope, xhat, scale, e_new, agg):
    def update(i):
        rows = pl.ds(i * BLOCK, BLOCK)
        act, slo = silu_parts(pre_of(rows))
        act = act.astype(BF16)
        hidden[rows, :] = act
        slope[rows, :] = slo
        xh, sc = norm_parts(mm(act, w2[...]) + b_ref[1:2, :])
        xhat[rows, :] = xh
        scale[rows, :] = sc
        new = (e_ref[rows, 0:128].astype(F32) + xh * g_ref[0:1, :]).astype(BF16)
        if e_new is not None:
            e_new[rows, :] = new
        return mm(spread_rows(rcv_ref[i], 256), new)

    blocks = e_ref.shape[0] // BLOCK
    gather(0)
    out = 0.0
    for i in range(blocks):
        if i + 1 < blocks:
            gather(i + 1)
        out = out + update(i)
    agg[...] = out


def node_forward(x, agg, wn1, wn2, b_ref, g_ref):
    joined = jnp.concatenate([x, agg.astype(BF16)], axis=1)
    act, slo = silu_parts(mm(joined, wn1[...]) + b_ref[2:3, :])
    act = act.astype(BF16)
    xh, sc = norm_parts(mm(act, wn2[...]) + b_ref[3:4, :])
    new = (x.astype(F32) + xh * g_ref[1:2, :]).astype(BF16)
    return new, (joined, act, slo, xh, sc)


def node_backward(cot, saved, wn1, wn2, g_ref):
    joined, act, slo, xh, sc = saved
    cot = cot.astype(F32)
    back = norm_back(cot, xh, sc, g_ref[1:2, :])
    back_b = back.astype(BF16)
    dpre = mm_nt(back_b, wn2[...]).astype(BF16).astype(F32) * slo
    dpre_b = dpre.astype(BF16)
    djoined = mm_nt(dpre_b, wn1[...]).astype(BF16)
    small = (total(dpre), total(back), total(cot * xh))
    return cot + djoined[:, 0:128].astype(F32), djoined[:, 128:256], (joined, dpre_b, act, back_b), small


def edge_backward(snd_ref, rcv_ref, w1, w2, g_ref, slope, xhat, scale, dagg, e_cot, e_grad, acc, dpres, backs, sums):
    acc[...] = jnp.zeros(acc.shape, F32)
    sums[...] = jnp.zeros(sums.shape, F32)

    def step(i, carry):
        rows = pl.ds(pl.multiple_of(i * BLOCK, BLOCK), BLOCK)
        cot = mm(pick_rows(rcv_ref[i], 256), dagg)
        if e_cot is not None:
            cot = (cot + e_cot[rows, :].astype(F32)).astype(BF16).astype(F32)
        xh = xhat[rows, :]
        back = norm_back(cot, xh, scale[rows, :], g_ref[0:1, :])
        back_b = back.astype(BF16)
        dpre = mm_nt(back_b, w2[...]).astype(BF16).astype(F32) * slope[rows, :]
        dpre_b = dpre.astype(BF16)
        djoined = mm_nt(dpre_b, w1[...]).astype(BF16)
        e_grad[rows, :] = (cot + djoined[:, 0:128].astype(F32)).astype(BF16)
        acc[...] += mm(spread_rows(snd_ref[i], 768), djoined[:, 128:256])
        acc[0:256, :] += mm(spread_rows(rcv_ref[i], 256), djoined[:, 256:384])
        dpres[rows, :] = dpre_b
        backs[rows, :] = back_b
        sums[0:1, :] += total(dpre)
        sums[1:2, :] += total(back)
        sums[2:3, :] += total(cot * xh)
        return carry

    lax.fori_loop(0, slope.shape[0] // BLOCK, step, 0, unroll=True)


def weight_grads(node_ops, joined, dpres, hidden, backs, grads):
    joined_n, dpre_n, act_n, back_n = node_ops
    first = mm_tn(dpres[...], joined[...])
    for k in range(3):
        grads[128 * k : 128 * k + 128, :] = jnp.transpose(first[:, 128 * k : 128 * k + 128]).astype(BF16)
    grads[384:512, :] = jnp.transpose(mm_tn(backs[...], hidden[...])).astype(BF16)
    grads[512:768, :] = mm_tn(joined_n, dpre_n).astype(BF16)
    grads[768:896, :] = mm_tn(act_n, back_n).astype(BF16)


def own_kernel(snd_ref, rcv_ref, x_ref, e_ref, w1, b_ref, joined, pre_own):
    for i in range(e_ref.shape[0] // BLOCK):
        rows = pl.ds(i * BLOCK, BLOCK)
        gather_own(i, snd_ref, rcv_ref, x_ref, e_ref, joined)
        pre_own[rows, :] = mm(joined[rows, :], w1[1]) + b_ref[1, 0:1, :]


def grads_kernel(
    joined_n, dpre_n, act_n, back_n, halo, dpres, hidden, backs, tail, joined, x_ref, agg_b, wn1, wn2, b_ref, g_ref,
    grads, *node_saved,
):
    first = joined[...]
    first = jnp.concatenate([first[:, 0:128], first[:, 128:256] + halo[...], first[:, 256:384]], axis=1)
    weight_grads((joined_n[...], dpre_n[...], act_n[...], back_n[...]), first, dpres, hidden, backs, grads)
    grads[896:GRAD_ROWS, :] = tail[...]
    _, saved = node_forward(x_ref[...], agg_b[...], wn1.at[0], wn2.at[0], b_ref.at[0], g_ref.at[0])
    for out, value in zip(node_saved, saved):
        out[...] = value


def small_rows(sums, small):
    tail = jnp.concatenate(
        [sums[0:2, :], small[0], small[1], sums[2:3, :], small[2], jnp.zeros((GRAD_ROWS - 902, H), F32)], axis=0
    )
    return tail.astype(BF16)


def first_kernel(
    snd_ref, rcv_ref, send_ref, x_ref, r0, r1, r2, r3, e_ref, w1, w2, wn1, wn2, b_ref, g_ref,
    joined, hidden, slope, xhat, scale, e_new, agg_b, x_new, o0, o1, o2, o3, table, agg,
):
    w1, w2, wn1, wn2, b_ref, g_ref = (r.at[0] for r in (w1, w2, wn1, wn2, b_ref, g_ref))
    fill_table(table, x_ref, (r0, r1, r2, r3))

    def gather(i):
        rows = pl.ds(i * BLOCK, BLOCK)
        joined[rows, 0:128] = e_ref[rows, :]
        joined[rows, 128:256] = mm(pick_rows(snd_ref[i], 768), table[...]).astype(BF16)
        joined[rows, 256:384] = mm(pick_rows(rcv_ref[i], 256), table[0:256, :]).astype(BF16)

    def pre_of(rows):
        return mm(joined[rows, :], w1[...]) + b_ref[0:1, :]

    edge_forward(gather, pre_of, rcv_ref, e_ref, w2, b_ref, g_ref, hidden, slope, xhat, scale, e_new, agg)
    new, saved = node_forward(x_ref[...], agg[...], wn1, wn2, b_ref, g_ref)
    agg_b[...] = agg[...].astype(BF16)
    x_new[...] = new
    write_sends(send_ref, new, (o0, o1, o2, o3))


def last_kernel(
    snd_ref, rcv_ref, x_ref, r0, r1, r2, r3, joined, pre_own, w1, w2, wn1, wn2, b_ref, g_ref, cot_ref,
    x_new, e_grad, x_grad, c0, c1, c2, c3, joined_n, dpre_n, act_n, back_n, halo, dpres, hidden, backs, tail,
    table, agg, slope, xhat, scale, acc, sums,
):
    w1, w2, wn1, wn2, b_ref, g_ref = (r.at[1] for r in (w1, w2, wn1, wn2, b_ref, g_ref))
    fill_table(table, x_ref, (r0, r1, r2, r3))

    def gather(i):
        picked = mm(pick_rows(snd_ref[i] - 256, 512), table[256:768, :])
        halo[pl.ds(i * BLOCK, BLOCK), :] = picked.astype(BF16)

    def pre_of(rows):
        return pre_own[rows, :] + mm(halo[rows, :], w1[128:256, :])

    edge_forward(gather, pre_of, rcv_ref, joined, w2, b_ref, g_ref, hidden, slope, xhat, scale, None, agg)
    new, saved = node_forward(x_ref[...], agg[...], wn1, wn2, b_ref, g_ref)
    x_new[...] = new
    dx, dagg, node_ops, small = node_backward(cot_ref[...], saved, wn1, wn2, g_ref)
    for out, op in zip((joined_n, dpre_n, act_n, back_n), node_ops):
        out[...] = op
    edge_backward(snd_ref, rcv_ref, w1, w2, g_ref, slope, xhat, scale, dagg, None, e_grad, acc, dpres, backs, sums)
    tail[...] = small_rows(sums, small)
    x_grad[...] = dx + acc[0:256, :]
    write_backs(acc, (c0, c1, c2, c3))


def back_kernel(
    snd_ref, rcv_ref, send_ref, n0, n1, n2, n3, n4, own_ref, t0, t1, t2, t3, joined, hidden, slope, xhat, scale, e_cot, late,
    w1, w2, wn1, wn2, b_ref, g_ref,
    e_grad, x_grad, c0, c1, c2, c3, grads, acc, dpres, backs, sums,
):
    w1, w2, wn1, wn2, b_ref, g_ref = (r.at[0] for r in (w1, w2, wn1, wn2, b_ref, g_ref))
    grads[GRAD_ROWS:, :] = late[...]
    cot = (own_ref[...] + add_returns(send_ref, (t0, t1, t2, t3))).astype(BF16)
    saved = tuple(r[...] for r in (n0, n1, n2, n3, n4))
    dx, dagg, node_ops, small = node_backward(cot, saved, wn1, wn2, g_ref)
    edge_backward(snd_ref, rcv_ref, w1, w2, g_ref, slope, xhat, scale, dagg, e_cot, e_grad, acc, dpres, backs, sums)
    weight_grads(node_ops, joined, dpres, hidden, backs, grads)
    grads[896:GRAD_ROWS, :] = small_rows(sums, small)
    x_grad[...] = dx + acc[0:256, :]
    write_backs(acc, (c0, c1, c2, c3))


def finish_kernel(send_ref, own_ref, t0, t1, t2, t3, o_ref):
    o_ref[...] = (own_ref[...] + add_returns(send_ref, (t0, t1, t2, t3))).astype(BF16)


def shape(*dims, dtype=F32):
    return jax.ShapeDtypeStruct(dims, dtype)


SMEM = pltpu.SMEM
VMEM = pltpu.VMEM
HBM = pltpu.HBM


def call(kernel, outs, scratch, args, name, spaces=None, sems=0):
    spaces = spaces or [VMEM] * len(args)
    args = [pltpu.with_memory_space_constraint(a, m) if m is HBM else a for a, m in zip(args, spaces)]
    extra = [pltpu.SemaphoreType.DMA((sems,))] if sems else []
    return pl.pallas_call(
        kernel,
        out_shape=outs,
        in_specs=[pl.BlockSpec(memory_space=m) for m in spaces],
        out_specs=[pl.BlockSpec(memory_space=VMEM)] * len(outs),
        scratch_shapes=[s if s.__class__ is not jax.ShapeDtypeStruct else VMEM(s.shape, s.dtype) for s in scratch] + extra,
        compiler_params=pltpu.CompilerParams(vmem_limit_bytes=VMEM_LIMIT),
        name=name,
    )(*args)


def swaps(axis, first):
    size = lax.axis_size(axis)
    return [p for i in range(first, size - 1, 2) for p in ((i, i + 1), (i + 1, i))]


def exchange(blocks):
    plan = (("dom", 0), ("dom", 1), ("group", 0), ("group", 1))
    return [lax.ppermute(b, axis, swaps(axis, first)) for b, (axis, first) in zip(blocks, plan)]


def fold_kernel(x_ref, *refs):
    o_ref = refs[-1]
    out = jnp.sum(x_ref[...].astype(F32), axis=0).astype(BF16)
    for k in range(o_ref.shape[0]):
        o_ref[k] = out


def unpack_kernel(scale, x_ref, *outs):
    for out, (a, b) in zip(outs, CUTS):
        for l in range(2):
            out[l] = x_ref[GRAD_ROWS * l + a : GRAD_ROWS * l + b, :].astype(F32) * scale


def swap_tiles(x, axis):
    return lax.all_to_all(x, axis, split_axis=0, concat_axis=0, tiled=True)


def reduce_grads(packed, scale, first, second):
    dom, group = lax.axis_size("dom"), lax.axis_size("group")
    rows = packed.shape[0] // dom
    tiles = swap_tiles(packed.reshape(dom, rows, H), "dom")
    (tiles,) = call(fold_kernel, [shape(group, rows, H, dtype=BF16)], [], (tiles, *first), "fold_dom")
    tiles = swap_tiles(tiles, "group")
    (tiles,) = call(fold_kernel, [shape(dom, rows, H, dtype=BF16)], [], (tiles, *second), "fold_group")
    whole = swap_tiles(tiles, "dom").reshape(dom * rows, H)
    return call(partial(unpack_kernel, scale), [shape(2, b - a, H) for a, b in CUTS], [], (whole,), "unpack")


def shards(nodes, edges, node_cot, send_index, halo_count, senders, receivers, edge_in_w, edge_out_w, node_in_w, node_out_w, biases, gains):
    x0 = nodes[0]
    e0 = edges[0]
    send = send_index[0]
    n_edge = e0.shape[0]
    snd = senders[0].reshape(n_edge // BLOCK, 1, BLOCK)
    rcv = receivers[0].reshape(n_edge // BLOCK, 1, BLOCK)
    weights = (edge_in_w, edge_out_w, node_in_w, node_out_w, biases, gains)
    rows4 = [shape(H, H, dtype=BF16)] * 4
    residuals = [
        shape(n_edge, 3 * H, dtype=BF16),
        shape(n_edge, H, dtype=BF16),
        shape(n_edge, H),
        shape(n_edge, H),
        shape(n_edge, 1),
    ]
    low = shape(n_edge, H, dtype=BF16)
    small = shape(256, H, dtype=BF16)
    operands = [shape(256, 2 * H, dtype=BF16), small, small, small, low, low, low, low, shape(GRAD_ROWS - 896, H, dtype=BF16)]
    table = shape(768, H, dtype=BF16)

    *sent, send, x0 = call(
        sends_kernel,
        rows4 + [shape(4, H, dtype=jnp.int32), shape(256, H, dtype=BF16)],
        [],
        (send, x0),
        "sends",
        [HBM, HBM],
        2,
    )
    raw = (snd, rcv, e0, node_cot[0], *weights)
    loaded = call(
        load_kernel,
        [shape(*a.shape, dtype=a.dtype) for a in raw],
        [SMEM((1, 4), jnp.int32)],
        (halo_count, sent[0], *raw),
        "load",
        [HBM, VMEM] + [HBM] * len(raw),
        1 + len(raw),
    )
    snd, rcv, e0, cot, *weights = loaded
    got = exchange(sent)
    out = call(
        first_kernel,
        residuals + [shape(n_edge, H, dtype=BF16), shape(256, H, dtype=BF16), shape(256, H, dtype=BF16)] + rows4,
        [table, shape(256, H)],
        (snd, rcv, send, x0, *got, e0, *weights),
        "layer0",
    )
    saved, (e1, agg0, x1), sent = out[:5], out[5:8], out[8:]
    got = exchange(sent)
    joined1, pre1 = call(
        own_kernel,
        [residuals[0], shape(n_edge, H)],
        [],
        (snd, rcv, x1, e1, weights[0], weights[4]),
        "own1",
    )
    out = call(
        last_kernel,
        [shape(256, H, dtype=BF16), shape(n_edge, H, dtype=BF16), shape(256, H)] + rows4 + operands,
        [table, shape(256, H)] + residuals[2:] + [shape(768, H), shape(8, H)],
        (snd, rcv, x1, *got, joined1, pre1, *weights, cot),
        "layer1",
    )
    nodes_out, e_cot, own = out[:3]
    back = exchange(out[3:7])
    grads1, *node0 = call(
        grads_kernel,
        [shape(GRAD_ROWS, H, dtype=BF16), shape(256, 2 * H, dtype=BF16), small, shape(256, H), shape(256, H), shape(256, 1)],
        [],
        (*out[7:], joined1, x0, agg0, *weights[2:]),
        "wgrad1",
    )
    out = call(
        back_kernel,
        [shape(n_edge, H, dtype=BF16), shape(256, H)] + rows4 + [shape(2 * GRAD_ROWS, H, dtype=BF16)],
        [shape(768, H), low, low, shape(8, H)],
        (snd, rcv, send, *node0, own, *back, *saved, e_cot, grads1, *weights),
        "back0",
    )
    edge_grad, own = out[:2]
    packed = out[6]
    back = exchange(out[2:6])
    (node_grad,) = call(finish_kernel, [shape(256, H, dtype=BF16)], [], (send, own, *back), "finish")

    scale = (lax.axis_size("dom") * lax.axis_size("group") * x0.shape[0]) ** (-0.5)
    grads = reduce_grads(packed, scale, back[:2], back[2:3])
    return (nodes_out[None], node_grad[None], edge_grad[None], *grads)


def solution(mesh):
    part = ("dom", "group")
    in_specs = (P(part),) * 7 + (P(),) * 6
    out_specs = (P(part),) * 3 + (P(),) * 6
    return jax.shard_map(shards, mesh=mesh, in_specs=in_specs, out_specs=out_specs, check_vma=False)
```

```python
from functools import partial

import jax
import jax.numpy as jnp
from jax import lax
from jax.experimental import pallas as pl
from jax.experimental.pallas import tpu as pltpu
from jax.sharding import PartitionSpec as P

H = 128
BLOCK = 768
GRAD_ROWS = 1024
VMEM_LIMIT = 28 << 20
CUTS = ((0, 384), (384, 512), (512, 768), (768, 896), (896, 900), (900, 902))
F32 = jnp.float32
BF16 = jnp.bfloat16


def mm(a, b):
    return lax.dot_general(a, b, (((1,), (0,)), ((), ())), preferred_element_type=F32)


def mm_nt(a, b):
    return lax.dot_general(a, b, (((1,), (1,)), ((), ())), preferred_element_type=F32)


def mm_tn(a, b):
    return lax.dot_general(a, b, (((0,), (0,)), ((), ())), preferred_element_type=F32)


def column(row):
    return jnp.transpose(jnp.broadcast_to(row, (8, row.shape[1])))[:, :1]


def hot(mask):
    return jnp.where(mask, 1.0, 0.0).astype(BF16)


def pick_rows(row, width):
    col = column(row)
    return hot(lax.broadcasted_iota(jnp.int32, (row.shape[1], width), 1) == col)


def spread_rows(row, width):
    return hot(lax.broadcasted_iota(jnp.int32, (width, row.shape[1]), 0) == row)


def slot_ids(ids, counts):
    out = ids
    end = 256
    for k in range(3):
        end = end + counts[k]
        out = out + jnp.where(ids >= end, 128 - counts[k], 0)
    return out


def silu_parts(pre):
    sig = 0.5 * jnp.tanh(0.5 * pre) + 0.5
    return pre * sig, sig * (1.0 + pre * (1.0 - sig))


def norm_parts(mapped):
    centre = mapped - jnp.mean(mapped, axis=-1, keepdims=True)
    spread = jnp.mean(centre * centre, axis=-1, keepdims=True)
    scale = lax.rsqrt(spread + 1e-05)
    return centre * scale, scale


def norm_back(cot, xhat, scale, gain):
    grad = cot * gain
    first = jnp.mean(grad, axis=-1, keepdims=True)
    second = jnp.mean(grad * xhat, axis=-1, keepdims=True)
    return scale * (grad - first - xhat * second)


def total(x):
    return jnp.sum(x, axis=0, keepdims=True)


def sides():
    p = lax.axis_index("dom") % 2
    g = lax.axis_index("group") % 2
    return (p, 1 - p), (1 - p, p), (2 + g, 3 - g), (3 - g, 2 + g)


def write_sends(send_ref, rows, outs):
    for (src, _), out in zip(sides(), outs):
        picked = mm(pick_rows(send_ref[pl.ds(src, 1), :], 256), rows)
        out[...] = picked.astype(BF16)


def add_returns(send_ref, rets):
    out = jnp.zeros((256, H), F32)
    for (src, _), ret in zip(sides(), rets):
        out = out + mm(spread_rows(send_ref[pl.ds(src, 1), :], 256), ret[...])
    return out


def slot_rows(slot):
    return pl.ds(pl.multiple_of(256 + 128 * slot, 128), 128)


def fill_table(table, x_ref, got):
    table[0:256, :] = x_ref[...]
    for (_, dst), r in zip(sides(), got):
        table[slot_rows(dst), :] = r[...]


def write_backs(acc, outs):
    for (_, dst), out in zip(sides(), outs):
        out[...] = acc[slot_rows(dst), :].astype(BF16)


def fetch(pairs, sems):
    copies = [pltpu.make_async_copy(src, dst, sems.at[i]) for i, (src, dst) in enumerate(pairs)]
    for c in copies:
        c.start()
    return copies


def sends_kernel(send_hbm, x_hbm, o0, o1, o2, o3, send_ref, x_ref, sems):
    for c in fetch(((send_hbm, send_ref), (x_hbm, x_ref)), sems):
        c.wait()
    write_sends(send_ref, x_ref[...], (o0, o1, o2, o3))


def load_kernel(cnt_hbm, token, *refs):
    cnt_ref, sems = refs[-2:]
    n = len(refs) // 2 - 1
    copies = fetch(((cnt_hbm, cnt_ref), *zip(refs[:n], refs[n:-2])), sems)
    for c in copies:
        c.wait()
    snd_ref = refs[n]
    snd_ref[...] = slot_ids(snd_ref[...], [cnt_ref[0, k] for k in range(3)])


def gather_own(i, snd_ref, rcv_ref, x_ref, e_ref, joined):
    rows = pl.ds(i * BLOCK, BLOCK)
    joined[rows, 0:128] = e_ref[rows, :]
    joined[rows, 128:256] = mm(pick_rows(snd_ref[i], 256), x_ref[0:256, :]).astype(BF16)
    joined[rows, 256:384] = mm(pick_rows(rcv_ref[i], 256), x_ref[0:256, :]).astype(BF16)


def edge_forward(gather, pre_of, rcv_ref, e_ref, w2, b_ref, g_ref, hidden, slope, xhat, scale, e_new, agg):
    def update(i):
        rows = pl.ds(i * BLOCK, BLOCK)
        act, slo = silu_parts(pre_of(rows))
        act = act.astype(BF16)
        hidden[rows, :] = act
        slope[rows, :] = slo
        xh, sc = norm_parts(mm(act, w2[...]) + b_ref[1:2, :])
        xhat[rows, :] = xh
        scale[rows, :] = sc
        new = (e_ref[rows, 0:128].astype(F32) + xh * g_ref[0:1, :]).astype(BF16)
        if e_new is not None:
            e_new[rows, :] = new
        return mm(spread_rows(rcv_ref[i], 256), new)

    blocks = e_ref.shape[0] // BLOCK
    gather(0)
    out = 0.0
    for i in range(blocks):
        if i + 1 < blocks:
            gather(i + 1)
        out = out + update(i)
    agg[...] = out


def node_forward(x, agg, wn1, wn2, b_ref, g_ref):
    joined = jnp.concatenate([x, agg.astype(BF16)], axis=1)
    act, slo = silu_parts(mm(joined, wn1[...]) + b_ref[2:3, :])
    act = act.astype(BF16)
    xh, sc = norm_parts(mm(act, wn2[...]) + b_ref[3:4, :])
    new = (x.astype(F32) + xh * g_ref[1:2, :]).astype(BF16)
    return new, (joined, act, slo, xh, sc)


def node_backward(cot, saved, wn1, wn2, g_ref):
    joined, act, slo, xh, sc = saved
    cot = cot.astype(F32)
    back = norm_back(cot, xh, sc, g_ref[1:2, :])
    back_b = back.astype(BF16)
    dpre = mm_nt(back_b, wn2[...]).astype(BF16).astype(F32) * slo
    dpre_b = dpre.astype(BF16)
    djoined = mm_nt(dpre_b, wn1[...]).astype(BF16)
    small = (total(dpre), total(back), total(cot * xh))
    return cot + djoined[:, 0:128].astype(F32), djoined[:, 128:256], (joined, dpre_b, act, back_b), small


def edge_backward(snd_ref, rcv_ref, w1, w2, g_ref, slope, xhat, scale, dagg, e_cot, e_grad, acc, dpres, backs, sums):
    acc[...] = jnp.zeros(acc.shape, F32)
    sums[...] = jnp.zeros(sums.shape, F32)

    def step(i, carry):
        rows = pl.ds(pl.multiple_of(i * BLOCK, BLOCK), BLOCK)
        cot = mm(pick_rows(rcv_ref[i], 256), dagg)
        if e_cot is not None:
            cot = (cot + e_cot[rows, :].astype(F32)).astype(BF16).astype(F32)
        xh = xhat[rows, :]
        back = norm_back(cot, xh, scale[rows, :], g_ref[0:1, :])
        back_b = back.astype(BF16)
        dpre = mm_nt(back_b, w2[...]).astype(BF16).astype(F32) * slope[rows, :]
        dpre_b = dpre.astype(BF16)
        djoined = mm_nt(dpre_b, w1[...]).astype(BF16)
        e_grad[rows, :] = (cot + djoined[:, 0:128].astype(F32)).astype(BF16)
        acc[...] += mm(spread_rows(snd_ref[i], 768), djoined[:, 128:256])
        acc[0:256, :] += mm(spread_rows(rcv_ref[i], 256), djoined[:, 256:384])
        dpres[rows, :] = dpre_b
        backs[rows, :] = back_b
        sums[0:1, :] += total(dpre)
        sums[1:2, :] += total(back)
        sums[2:3, :] += total(cot * xh)
        return carry

    lax.fori_loop(0, slope.shape[0] // BLOCK, step, 0, unroll=True)


def weight_grads(node_ops, joined, dpres, hidden, backs, grads):
    joined_n, dpre_n, act_n, back_n = node_ops
    first = mm_tn(dpres[...], joined[...])
    for k in range(3):
        grads[128 * k : 128 * k + 128, :] = jnp.transpose(first[:, 128 * k : 128 * k + 128]).astype(BF16)
    grads[384:512, :] = jnp.transpose(mm_tn(backs[...], hidden[...])).astype(BF16)
    grads[512:768, :] = mm_tn(joined_n, dpre_n).astype(BF16)
    grads[768:896, :] = mm_tn(act_n, back_n).astype(BF16)


def own_kernel(snd_ref, rcv_ref, x_ref, e_ref, w1, b_ref, joined, pre_own):
    for i in range(e_ref.shape[0] // BLOCK):
        rows = pl.ds(i * BLOCK, BLOCK)
        gather_own(i, snd_ref, rcv_ref, x_ref, e_ref, joined)
        pre_own[rows, :] = mm(joined[rows, :], w1[1]) + b_ref[1, 0:1, :]


def grads_kernel(
    joined_n, dpre_n, act_n, back_n, halo, dpres, hidden, backs, tail, joined, x_ref, agg_b, wn1, wn2, b_ref, g_ref,
    grads, *node_saved,
):
    first = joined[...]
    first = jnp.concatenate([first[:, 0:128], first[:, 128:256] + halo[...], first[:, 256:384]], axis=1)
    weight_grads((joined_n[...], dpre_n[...], act_n[...], back_n[...]), first, dpres, hidden, backs, grads)
    grads[896:GRAD_ROWS, :] = tail[...]
    _, saved = node_forward(x_ref[...], agg_b[...], wn1.at[0], wn2.at[0], b_ref.at[0], g_ref.at[0])
    for out, value in zip(node_saved, saved):
        out[...] = value


def small_rows(sums, small):
    tail = jnp.concatenate(
        [sums[0:2, :], small[0], small[1], sums[2:3, :], small[2], jnp.zeros((GRAD_ROWS - 902, H), F32)], axis=0
    )
    return tail.astype(BF16)


def first_kernel(
    snd_ref, rcv_ref, send_ref, x_ref, r0, r1, r2, r3, e_ref, w1, w2, wn1, wn2, b_ref, g_ref,
    joined, hidden, slope, xhat, scale, e_new, agg_b, x_new, o0, o1, o2, o3, table, agg,
):
    w1, w2, wn1, wn2, b_ref, g_ref = (r.at[0] for r in (w1, w2, wn1, wn2, b_ref, g_ref))
    fill_table(table, x_ref, (r0, r1, r2, r3))

    def gather(i):
        rows = pl.ds(i * BLOCK, BLOCK)
        joined[rows, 0:128] = e_ref[rows, :]
        joined[rows, 128:256] = mm(pick_rows(snd_ref[i], 768), table[...]).astype(BF16)
        joined[rows, 256:384] = mm(pick_rows(rcv_ref[i], 256), table[0:256, :]).astype(BF16)

    def pre_of(rows):
        return mm(joined[rows, :], w1[...]) + b_ref[0:1, :]

    edge_forward(gather, pre_of, rcv_ref, e_ref, w2, b_ref, g_ref, hidden, slope, xhat, scale, e_new, agg)
    new, saved = node_forward(x_ref[...], agg[...], wn1, wn2, b_ref, g_ref)
    agg_b[...] = agg[...].astype(BF16)
    x_new[...] = new
    write_sends(send_ref, new, (o0, o1, o2, o3))


def last_kernel(
    snd_ref, rcv_ref, x_ref, r0, r1, r2, r3, joined, pre_own, w1, w2, wn1, wn2, b_ref, g_ref, cot_ref,
    x_new, e_grad, x_grad, c0, c1, c2, c3, joined_n, dpre_n, act_n, back_n, halo, dpres, hidden, backs, tail,
    table, agg, slope, xhat, scale, acc, sums,
):
    w1, w2, wn1, wn2, b_ref, g_ref = (r.at[1] for r in (w1, w2, wn1, wn2, b_ref, g_ref))
    fill_table(table, x_ref, (r0, r1, r2, r3))

    def gather(i):
        picked = mm(pick_rows(snd_ref[i] - 256, 512), table[256:768, :])
        halo[pl.ds(i * BLOCK, BLOCK), :] = picked.astype(BF16)

    def pre_of(rows):
        return pre_own[rows, :] + mm(halo[rows, :], w1[128:256, :])

    edge_forward(gather, pre_of, rcv_ref, joined, w2, b_ref, g_ref, hidden, slope, xhat, scale, None, agg)
    new, saved = node_forward(x_ref[...], agg[...], wn1, wn2, b_ref, g_ref)
    x_new[...] = new
    dx, dagg, node_ops, small = node_backward(cot_ref[...], saved, wn1, wn2, g_ref)
    for out, op in zip((joined_n, dpre_n, act_n, back_n), node_ops):
        out[...] = op
    edge_backward(snd_ref, rcv_ref, w1, w2, g_ref, slope, xhat, scale, dagg, None, e_grad, acc, dpres, backs, sums)
    tail[...] = small_rows(sums, small)
    x_grad[...] = dx + acc[0:256, :]
    write_backs(acc, (c0, c1, c2, c3))


def back_kernel(
    snd_ref, rcv_ref, send_ref, n0, n1, n2, n3, n4, own_ref, t0, t1, t2, t3, joined, hidden, slope, xhat, scale, e_cot, late,
    w1, w2, wn1, wn2, b_ref, g_ref,
    e_grad, x_grad, c0, c1, c2, c3, grads, acc, dpres, backs, sums,
):
    w1, w2, wn1, wn2, b_ref, g_ref = (r.at[0] for r in (w1, w2, wn1, wn2, b_ref, g_ref))
    grads[GRAD_ROWS:, :] = late[...]
    cot = (own_ref[...] + add_returns(send_ref, (t0, t1, t2, t3))).astype(BF16)
    saved = tuple(r[...] for r in (n0, n1, n2, n3, n4))
    dx, dagg, node_ops, small = node_backward(cot, saved, wn1, wn2, g_ref)
    edge_backward(snd_ref, rcv_ref, w1, w2, g_ref, slope, xhat, scale, dagg, e_cot, e_grad, acc, dpres, backs, sums)
    weight_grads(node_ops, joined, dpres, hidden, backs, grads)
    grads[896:GRAD_ROWS, :] = small_rows(sums, small)
    x_grad[...] = dx + acc[0:256, :]
    write_backs(acc, (c0, c1, c2, c3))


def finish_kernel(send_ref, own_ref, t0, t1, t2, t3, o_ref):
    o_ref[...] = (own_ref[...] + add_returns(send_ref, (t0, t1, t2, t3))).astype(BF16)


def shape(*dims, dtype=F32):
    return jax.ShapeDtypeStruct(dims, dtype)


SMEM = pltpu.SMEM
VMEM = pltpu.VMEM
HBM = pltpu.HBM


def call(kernel, outs, scratch, args, name, spaces=None, sems=0):
    spaces = spaces or [VMEM] * len(args)
    args = [pltpu.with_memory_space_constraint(a, m) if m is HBM else a for a, m in zip(args, spaces)]
    extra = [pltpu.SemaphoreType.DMA((sems,))] if sems else []
    return pl.pallas_call(
        kernel,
        out_shape=outs,
        in_specs=[pl.BlockSpec(memory_space=m) for m in spaces],
        out_specs=[pl.BlockSpec(memory_space=VMEM)] * len(outs),
        scratch_shapes=[s if s.__class__ is not jax.ShapeDtypeStruct else VMEM(s.shape, s.dtype) for s in scratch] + extra,
        compiler_params=pltpu.CompilerParams(vmem_limit_bytes=VMEM_LIMIT),
        name=name,
    )(*args)


def swaps(axis, first):
    size = lax.axis_size(axis)
    return [p for i in range(first, size - 1, 2) for p in ((i, i + 1), (i + 1, i))]


def exchange(blocks):
    plan = (("dom", 0), ("dom", 1), ("group", 0), ("group", 1))
    return [lax.ppermute(b, axis, swaps(axis, first)) for b, (axis, first) in zip(blocks, plan)]


def fold_kernel(x_ref, *refs):
    o_ref = refs[-1]
    out = jnp.sum(x_ref[...].astype(F32), axis=0).astype(BF16)
    for k in range(o_ref.shape[0]):
        o_ref[k] = out


def unpack_kernel(scale, x_ref, *outs):
    for out, (a, b) in zip(outs, CUTS):
        for l in range(2):
            out[l] = x_ref[GRAD_ROWS * l + a : GRAD_ROWS * l + b, :].astype(F32) * scale


def swap_tiles(x, axis):
    return lax.all_to_all(x, axis, split_axis=0, concat_axis=0, tiled=True)


def reduce_grads(packed, scale, first, second):
    dom, group = lax.axis_size("dom"), lax.axis_size("group")
    rows = packed.shape[0] // dom
    tiles = swap_tiles(packed.reshape(dom, rows, H), "dom")
    (tiles,) = call(fold_kernel, [shape(group, rows, H, dtype=BF16)], [], (tiles, *first), "fold_dom")
    tiles = swap_tiles(tiles, "group")
    (tiles,) = call(fold_kernel, [shape(dom, rows, H, dtype=BF16)], [], (tiles, *second), "fold_group")
    whole = swap_tiles(tiles, "dom").reshape(dom * rows, H)
    return call(partial(unpack_kernel, scale), [shape(2, b - a, H) for a, b in CUTS], [], (whole,), "unpack")


def shards(nodes, edges, node_cot, send_index, halo_count, senders, receivers, edge_in_w, edge_out_w, node_in_w, node_out_w, biases, gains):
    x0 = nodes[0]
    e0 = edges[0]
    send = send_index[0]
    n_edge = e0.shape[0]
    snd = senders[0].reshape(n_edge // BLOCK, 1, BLOCK)
    rcv = receivers[0].reshape(n_edge // BLOCK, 1, BLOCK)
    weights = (edge_in_w, edge_out_w, node_in_w, node_out_w, biases, gains)
    rows4 = [shape(H, H, dtype=BF16)] * 4
    residuals = [
        shape(n_edge, 3 * H, dtype=BF16),
        shape(n_edge, H, dtype=BF16),
        shape(n_edge, H),
        shape(n_edge, H),
        shape(n_edge, 1),
    ]
    low = shape(n_edge, H, dtype=BF16)
    small = shape(256, H, dtype=BF16)
    operands = [shape(256, 2 * H, dtype=BF16), small, small, small, low, low, low, low, shape(GRAD_ROWS - 896, H, dtype=BF16)]
    table = shape(768, H, dtype=BF16)

    *sent, send, x0 = call(
        sends_kernel,
        rows4 + [shape(4, H, dtype=jnp.int32), shape(256, H, dtype=BF16)],
        [],
        (send, x0),
        "sends",
        [HBM, HBM],
        2,
    )
    raw = (snd, rcv, e0, node_cot[0], *weights)
    loaded = call(
        load_kernel,
        [shape(*a.shape, dtype=a.dtype) for a in raw],
        [SMEM((1, 4), jnp.int32)],
        (halo_count, sent[0], *raw),
        "load",
        [HBM, VMEM] + [HBM] * len(raw),
        1 + len(raw),
    )
    snd, rcv, e0, cot, *weights = loaded
    got = exchange(sent)
    out = call(
        first_kernel,
        residuals + [shape(n_edge, H, dtype=BF16), shape(256, H, dtype=BF16), shape(256, H, dtype=BF16)] + rows4,
        [table, shape(256, H)],
        (snd, rcv, send, x0, *got, e0, *weights),
        "layer0",
    )
    saved, (e1, agg0, x1), sent = out[:5], out[5:8], out[8:]
    got = exchange(sent)
    joined1, pre1 = call(
        own_kernel,
        [residuals[0], shape(n_edge, H)],
        [],
        (snd, rcv, x1, e1, weights[0], weights[4]),
        "own1",
    )
    out = call(
        last_kernel,
        [shape(256, H, dtype=BF16), shape(n_edge, H, dtype=BF16), shape(256, H)] + rows4 + operands,
        [table, shape(256, H)] + residuals[2:] + [shape(768, H), shape(8, H)],
        (snd, rcv, x1, *got, joined1, pre1, *weights, cot),
        "layer1",
    )
    nodes_out, e_cot, own = out[:3]
    back = exchange(out[3:7])
    grads1, *node0 = call(
        grads_kernel,
        [shape(GRAD_ROWS, H, dtype=BF16), shape(256, 2 * H, dtype=BF16), small, shape(256, H), shape(256, H), shape(256, 1)],
        [],
        (*out[7:], joined1, x0, agg0, *weights[2:]),
        "wgrad1",
    )
    out = call(
        back_kernel,
        [shape(n_edge, H, dtype=BF16), shape(256, H)] + rows4 + [shape(2 * GRAD_ROWS, H, dtype=BF16)],
        [shape(768, H), low, low, shape(8, H)],
        (snd, rcv, send, *node0, own, *back, *saved, e_cot, grads1, *weights),
        "back0",
    )
    edge_grad, own = out[:2]
    packed = out[6]
    back = exchange(out[2:6])
    (node_grad,) = call(finish_kernel, [shape(256, H, dtype=BF16)], [], (send, own, *back), "finish")

    scale = (lax.axis_size("dom") * lax.axis_size("group") * x0.shape[0]) ** (-0.5)
    grads = reduce_grads(packed, scale, back[2:], ())
    return (nodes_out[None], node_grad[None], edge_grad[None], *grads)


def solution(mesh):
    part = ("dom", "group")
    in_specs = (P(part),) * 7 + (P(),) * 6
    out_specs = (P(part),) * 3 + (P(),) * 6
    return jax.shard_map(shards, mesh=mesh, in_specs=in_specs, out_specs=out_specs, check_vma=False)
```
